32 devices in a mesh: gx: 4 (over y, x), gy: 2 (over core), gz: 4 (over z).
Axes of the slice: x: 2, y: 2, z: 4, core: 2. Of those that a mesh axis runs over, the one named last changes fastest.
Arguments:
- volume: bfloat16 [32, 64, 64, 32], P('gx', 'gy', 'gz'), may hold values from -6 to 6
- conv_in: bfloat16 [3, 3, 3, 32, 32], replicated, may hold values from -0.21875 to 0.21875
- conv_out: bfloat16 [3, 3, 3, 32, 32], replicated, may hold values from -0.21875 to 0.21875
- norm_gain: float32 [256], replicated, may hold values from 0.1 to 1.9
- q_weight: bfloat16 [256, 256], replicated, may hold values from -3 to 3
- kv_weight: bfloat16 [256, 512], replicated, may hold values from -0.375 to 0.375
- out_weight: bfloat16 [256, 256], replicated, may hold values from -0.375 to 0.375
- up_weight: bfloat16 [256, 256], replicated, may hold values from -0.375 to 0.375
Outputs:
- joined_out: bfloat16 [32, 64, 64, 32], P('gx', 'gy', 'gz')
The draws below stay inside these ranges and needn't reach their ends.
All inputs are finite; a program needn't handle non-finite values.
Results may differ from the reference program's by a relative error of at most 0.012.
The reference program's roundings to bfloat16 on the way (of `encoded`, `normed`, `attended`, `mixture` and `joined`) count: a program that leaves them out, or rounds other values in their place, can miss the bound.
Values may be sent and summed in bfloat16 or wider, within the bound.
No kernel may reach another device: no remote copies, remote signals or barrier semaphores. Data moves between devices by JAX's collectives and lax.ppermute only.
A program may use at most 64 MiB of HBM per device.

```python
import math
import jax
import jax.numpy as jnp
from jax import lax

C = 32
HEADS = 8
F = 256
NX = 32
NY = 64
NZ = 64


def draw_q_weight(key, part):
    factor = 2.5
    values = jax.random.normal(key, (F, F), jnp.float32) * (factor / math.sqrt(F))
    return jnp.clip(values, -3.0, 3.0).astype(jnp.bfloat16)


def levels(stream_key, extent, cuts, smallest, top_value):
    factor_of = 1.0
    for dim, shards_of in cuts:
        steps = jax.random.uniform(jax.random.fold_in(jax.random.fold_in(stream_key, 6), dim), (shards_of,), jnp.float32, smallest / len(cuts), top_value / len(cuts))
        factor_of = factor_of * jnp.repeat(jnp.exp(steps), extent[dim] // shards_of).reshape((-1,) + (1,) * (len(extent) - 1 - dim))
    return factor_of


def scatter_about(own_key, shape, deviation, bound, pieces=(), held_as=jnp.bfloat16):
    entries = jax.random.normal(own_key, shape, jnp.float32) * deviation
    if len(pieces) > 0:
        entries = levels(own_key, shape, pieces, -0.22, 0.18) * entries
    return jnp.clip(entries, min=-bound, max=bound).astype(held_as)


def setup_inputs(seed: int = 0) -> dict:
    seeds = jax.random.split(jax.random.key(seed), 9)
    return {
        "volume": scatter_about(seeds[0], (NX, NY, NZ, C), 1.0, 6.0, ((0, 4), (1, 2), (2, 4))),
        "conv_in": scatter_about(seeds[1], (3, 3, 3, C, C), (27 * C) ** -0.5, 0.21875),
        "conv_out": scatter_about(seeds[2], (3, 3, 3, C, C), (27 * C) ** -0.5, 0.21875),
        "norm_gain": jnp.clip(1.0 + 0.18 * jax.random.normal(seeds[3], (F,), jnp.float32), 0.1, 1.9),
        "q_weight": draw_q_weight(jax.random.fold_in(seeds[8], 71), 0),
        "kv_weight": scatter_about(seeds[5], (F, 2 * F), F ** -0.5, 0.375),
        "out_weight": scatter_about(seeds[6], (F, F), F ** -0.5, 0.375),
        "up_weight": scatter_about(seeds[7], (F, F), F ** -0.5, 0.375),
    }


def convolve(volume_map, kernel):
    return lax.conv_general_dilated(volume_map[None], kernel, (1, 1, 1), 'SAME', dimension_numbers=('NDHWC', 'DHWIO', 'NDHWC'), preferred_element_type=jnp.float32)[0]

def tokenize(volume_map):
    extent_x, extent_y, extent_z, channels = volume_map.shape
    grid_cells = volume_map.reshape(extent_x // 8, 2, 4, extent_y // 8, 2, 4, extent_z // 8, 2, 4, channels).mean(axis=(2, 5, 8))
    grid_cells = grid_cells.transpose(0, 2, 4, 1, 3, 5, 6)
    return grid_cells.reshape(extent_x // 8 * (extent_y // 8) * (extent_z // 8), 8 * channels)

def spread_cells(token_rows, extent_x, extent_y, extent_z):
    channels = token_rows.shape[1] // 8
    grid_cells = token_rows.reshape(extent_x // 8, extent_y // 8, extent_z // 8, 2, 2, 2, channels).transpose(0, 3, 1, 4, 2, 5, 6)
    grid_cells = jnp.broadcast_to(grid_cells[:, :, None, :, :, None, :, :, None, :], (extent_x // 8, 2, 4, extent_y // 8, 2, 4, extent_z // 8, 2, 4, channels))
    return grid_cells.reshape(extent_x, extent_y, extent_z, channels)

def layer_norm(tokens, norm_gain):
    center = tokens - tokens.mean(axis=1, keepdims=True)
    spread = (center * center).mean(axis=1, keepdims=True)
    return (center * lax.rsqrt(spread + 1e-05) * norm_gain).astype(jnp.bfloat16)

def attention(queries, key_rows, value_rows):
    token_count = queries.shape[0]
    head_size = F // HEADS
    block_rows = math.gcd(token_count, 2048)

    def split_heads(matrix):
        return matrix.reshape(token_count, HEADS, head_size).transpose(1, 0, 2)

    def one_head(operands):
        head_query, head_keys, head_values = operands
        query_blocks = head_query.reshape(token_count // block_rows, block_rows, head_size)

        def one_block(query_block):
            scores = jnp.dot(query_block, head_keys.T, preferred_element_type=jnp.float32) * head_size ** (-0.5)
            row_peak = scores.max(axis=1, keepdims=True)
            weights = jnp.exp(scores - row_peak)
            numerator = jnp.dot(weights.astype(jnp.bfloat16), head_values, preferred_element_type=jnp.float32)
            return (numerator / weights.sum(axis=1, keepdims=True)).astype(jnp.bfloat16)
        return lax.map(one_block, query_blocks).reshape(token_count, head_size)
    result = lax.map(one_head, (split_heads(queries), split_heads(key_rows), split_heads(value_rows)))
    return result.transpose(1, 0, 2).reshape(token_count, F)

def reference(volume, conv_in, conv_out, norm_gain, q_weight, kv_weight, out_weight, up_weight):
    encoded = jax.nn.relu(convolve(volume, conv_in)).astype(jnp.bfloat16)
    tokens = tokenize(encoded.astype(jnp.float32))
    normed = layer_norm(tokens, norm_gain)
    queries = jnp.dot(normed, q_weight, preferred_element_type=jnp.float32).astype(jnp.bfloat16)
    key_value = jnp.dot(normed, kv_weight, preferred_element_type=jnp.float32).astype(jnp.bfloat16)
    attended = attention(queries, key_value[:, :F], key_value[:, F:])
    mixture = (tokens + jnp.dot(attended, out_weight, preferred_element_type=jnp.float32)).astype(jnp.bfloat16)
    upward = jnp.dot(mixture, up_weight, preferred_element_type=jnp.float32)
    joined = (encoded.astype(jnp.float32) + spread_cells(upward, NX, NY, NZ)).astype(jnp.bfloat16)
    return convolve(joined, conv_out).astype(jnp.bfloat16)
```

```python
import numpy as np

import jax
import jax.numpy as jnp
from jax import lax
from jax.experimental import pallas as pl
from jax.experimental.pallas import tpu as pltpu
from jax.sharding import PartitionSpec as P

HEADS = 8
AXES = ("gx", "gy", "gz")
OUT_Z = 6
IN_Z = 8

f32 = jnp.float32
bf16 = jnp.bfloat16


def exchange(low, high, axis):
    count = lax.axis_size(axis)
    if count == 1:
        return low, low
    if count == 2:
        mine = jnp.where(lax.axis_index(axis) == 0, high, low)
        other = lax.ppermute(mine, axis, [(0, 1), (1, 0)])
        return other, other
    below = lax.ppermute(high, axis, [(i, (i + 1) % count) for i in range(count)])
    above = lax.ppermute(low, axis, [((i + 1) % count, i) for i in range(count)])
    return below, above


def call(body, outs, scratch=(), in_smem=0, total=0):
    specs = [pl.BlockSpec(memory_space=pltpu.SMEM)] * in_smem + [
        pl.BlockSpec(memory_space=pltpu.VMEM)
    ] * (total - in_smem)
    return pl.pallas_call(
        body,
        out_shape=outs,
        in_specs=specs,
        scratch_shapes=list(scratch),
        name=body.__name__,
    )


def band_weights(kernel_in, kernel_out, up_weight, chan):
    width = up_weight.shape[0]

    def spread_weights(kin, kout, up, first, second, upx):
        for source, target in ((kin, first), (kout, second)):
            target[...] = jnp.zeros(target.shape, target.dtype)
            for tap in range(9):
                block = source[tap]
                for z in range(OUT_Z):
                    target[tap, z * chan : (z + 3) * chan, z * chan : (z + 1) * chan] = block
        for a in range(2):
            pieces = []
            for b in range(2):
                for c in range(2):
                    start = (a * 4 + b * 2 + c) * chan
                    pieces += [up[:, start : start + chan]] * 4
            upx[a] = jnp.concatenate(pieces, axis=1)

    banded = jax.ShapeDtypeStruct((9, IN_Z * chan, OUT_Z * chan), bf16)
    return call(
        spread_weights,
        (banded, banded, jax.ShapeDtypeStruct((2, width, 16 * chan), bf16)),
        total=3,
    )(
        kernel_in.reshape(9, 3 * chan, chan),
        kernel_out.reshape(9, 3 * chan, chan),
        up_weight,
    )


def pack_rows(volume, below, above):
    bx, by, bz, chan = volume.shape
    lanes = (bz + 4) * chan

    def pack(vol, zm, zp, rows, ylow, yhigh):
        own = vol[...].reshape(bx * by, bz * chan)
        full = jnp.concatenate([zm[...], own, zp[...]], axis=1)
        rows[...] = full
        planes = full.astype(f32).reshape(bx, by, lanes)
        ylow[...] = planes[:, :2].reshape(bx * 2, lanes).astype(bf16)
        yhigh[...] = planes[:, by - 2 :].reshape(bx * 2, lanes).astype(bf16)

    face = jax.ShapeDtypeStruct((bx * 2, lanes), bf16)
    return call(
        pack, (jax.ShapeDtypeStruct((bx * by, lanes), bf16), face, face), total=3
    )(volume, below, above)


def banded_conv(source, weights, sums, blocks, rows, stride, chan):
    outs = []
    for block in range(blocks):
        start = block * OUT_Z * chan
        for dy in range(3):
            total = None
            for dx in range(3):
                piece = source[dx * stride : dx * stride + rows, start : start + IN_Z * chan]
                part = jnp.dot(
                    piece.astype(bf16), weights[dx * 3 + dy], preferred_element_type=f32
                )
                total = part if total is None else total + part
            sums[dy, :rows, :] = total
        outs.append(sums[0, 0:rows, :] + sums[1, 1 : rows + 1, :] + sums[2, 2 : rows + 2, :])
    return outs


def encode(pos, rows_z, yfaces, xbelow, xabove, weights, shape, counts):
    bx, by, bz, chan = shape
    nx, ny, nz = counts
    lanes = (bz + 4) * chan
    stride = by + 8
    tall = (bx + 2) * stride
    blocks = (bz + 2) // OUT_Z
    ti, tj, tk = bx // 8, by // 8, bz // 8
    tokens = ti * tj * tk
    width = 8 * chan
    yparts = len(yfaces)

    def encode_rows(pos_ref, vz, *refs):
        yrefs = refs[:yparts]
        xm, xp, w, enc, tok, grid, sums, plane_sum = refs[yparts:]
        lane = lax.broadcasted_iota(jnp.int32, (1, lanes), 1)
        z_ok = ((lane >= 2 * chan) | (pos_ref[2] > 0)) & (
            (lane < (bz + 2) * chan) | (pos_ref[2] < nz - 1)
        )
        y_lo, y_hi = pos_ref[1] > 0, pos_ref[1] < ny - 1
        x_lo, x_hi = pos_ref[0] > 0, pos_ref[0] < nx - 1

        def put(row, value, ok=None):
            good = z_ok if ok is None else z_ok & ok
            grid[row : row + value.shape[0], :] = jnp.where(good, value.astype(f32), 0.0)

        for p in range(bx):
            base = (p + 2) * stride
            put(base + 2, vz[p * by : (p + 1) * by, :])
            ym = yrefs[0][...].astype(f32)[2 * p : 2 * p + 2]
            yp = yrefs[-1][...].astype(f32)[2 * p : 2 * p + 2]
            put(base, ym, y_lo)
            put(base + by + 2, yp, y_hi)
        for ref, first, ok in ((xm, 0, x_lo), (xp, bx + 2, x_hi)):
            tail = ref[2 * by :, :].astype(f32)
            for q in range(2):
                base = (first + q) * stride
                put(base + 2, ref[q * by : (q + 1) * by, :], ok)
                put(base, tail[2 * q : 2 * q + 2], ok & y_lo)
                last = 4 * (yparts - 1) + 2 * q
                put(base + by + 2, tail[last : last + 2], ok & y_hi)
        outs = banded_conv(grid, w, sums, blocks, tall, stride, chan)
        encoded = jnp.maximum(jnp.concatenate(outs, axis=1), 0.0).astype(bf16)
        enc[...] = encoded
        cells = encoded.astype(f32)
        rows_of = {}
        for i in range(ti):
            features = {}
            for a in range(2):
                x0 = 1 + 8 * i + 4 * a
                acc = cells[x0 * stride : (x0 + 1) * stride]
                for q in range(1, 4):
                    acc = acc + cells[(x0 + q) * stride : (x0 + q + 1) * stride]
                for g in range(2 * tk):
                    at = (1 + 4 * g) * chan
                    plane_sum[g] = acc[:, at : at + 4 * chan]
                for b in range(2):
                    for g in range(2 * tk):
                        part = None
                        for q in range(4):
                            line = plane_sum[g, pl.ds(1 + 4 * b + q, tj, stride=8), :]
                            part = line if part is None else part + line
                        s = part[:, :chan]
                        for q in range(1, 4):
                            s = s + part[:, q * chan : (q + 1) * chan]
                        features[a, b, g] = s * (1.0 / 64.0)
            for k in range(tk):
                rows_of[i, k] = jnp.concatenate(
                    [features[a, b, 2 * k + c] for a in range(2) for b in range(2) for c in range(2)],
                    axis=1,
                )
        tok[...] = jnp.concatenate(
            [rows_of[i, k] for i in range(ti) for k in range(tk)], axis=0
        ).astype(tok.dtype)

    return call(
        encode_rows,
        (
            jax.ShapeDtypeStruct((tall, (bz + 2) * chan), bf16),
            jax.ShapeDtypeStruct((tokens, width), f32),
        ),
        scratch=[
            pltpu.VMEM(((bx + 4) * stride, lanes), f32),
            pltpu.VMEM((3, tall + 8, OUT_Z * chan), f32),
            pltpu.VMEM((2 * tk, stride, 4 * chan), f32),
        ],
        in_smem=1,
        total=5 + yparts,
    )(pos, rows_z, *yfaces, xbelow, xabove, weights)


def sub_blocks(extent):
    out = [(0, 1, -1, extent // 8 - 1, 1)]
    for s in range(extent // 4):
        out.append((1 + 4 * s, 4, 0, s // 2, s % 2))
    out.append((extent + 1, 1, 1, 0, 0))
    return out


def attend_and_join(
    pos, gathered, gain, q_weight, kv_weight, out_weight, upx, encoded, weights, shape, counts
):
    bx, by, bz, chan = shape
    nx, ny, nz = counts
    stride = by + 8
    tall, low = (bx + 2) * stride, bx * stride
    ti, tj, tk = bx // 8, by // 8, bz // 8
    tokens = ti * tj * tk
    width = 8 * chan
    every = gathered.shape[0]
    asked = 27 * tokens
    head_size = width // HEADS
    wide = (bz + 2) * chan
    blocks = -(-bz // OUT_Z)
    padded = (blocks * OUT_Z + 2) * chan

    xs = sub_blocks(bx)
    zs = [(-1, tk - 1, (7 * chan, 8 * chan))]
    zs += [(0, k, (0, 8 * chan)) for k in range(tk)]
    zs += [(1, 0, (0, chan))]
    pick = np.zeros((len(xs) * len(zs) * stride, asked), np.float32)
    for xi, (_, _, dx, i, _) in enumerate(xs):
        for zi, (dz, k, _) in enumerate(zs):
            for first, many, dy, j, _ in sub_blocks(by):
                near = ((dx + 1) * 3 + dy + 1) * 3 + dz + 1
                row = (xi * len(zs) + zi) * stride + first
                pick[row : row + many, near * tokens + (i * tk + k) * tj + j] = 1.0

    def attend(
        pos_ref, g, gain_ref, qw, kvw, ow, upx_ref, sel, enc, w, out, normed_all, mine, mine_n, grid, sums
    ):
        t = g[...].astype(f32)
        center = t - jnp.mean(t, axis=1, keepdims=True)
        spread = jnp.mean(center * center, axis=1, keepdims=True)
        normed = (center * lax.rsqrt(spread + 1e-05) * gain_ref[...]).astype(bf16)
        normed_all[...] = normed.astype(f32)
        kv = jnp.dot(normed, kvw[...], preferred_element_type=f32).astype(bf16)
        keys, values = kv[:, :width], kv[:, width:]
        near = 0
        for dx in (-1, 0, 1):
            x = jnp.clip(pos_ref[0] + dx, 0, nx - 1)
            for dy in (-1, 0, 1):
                y = jnp.clip(pos_ref[1] + dy, 0, ny - 1)
                for dz in (-1, 0, 1):
                    z = jnp.clip(pos_ref[2] + dz, 0, nz - 1)
                    at = pl.multiple_of(((x * ny + y) * nz + z) * tokens, 8)
                    mine[near * tokens : (near + 1) * tokens, :] = g[pl.ds(at, tokens), :]
                    mine_n[near * tokens : (near + 1) * tokens, :] = normed_all[pl.ds(at, tokens), :]
                    near += 1
        q = jnp.dot(mine_n[...].astype(bf16), qw[...], preferred_element_type=f32).astype(bf16)
        lane = lax.broadcasted_iota(jnp.int32, (1, width), 1) // head_size
        attended = jnp.zeros((asked, width), f32)
        for h in range(HEADS):
            here = lane == h
            q_h = jnp.where(here, q, jnp.zeros_like(q))
            scores = (
                lax.dot_general(q_h, keys, (((1,), (1,)), ((), ())), preferred_element_type=f32)
                * head_size ** (-0.5)
            )
            e = jnp.exp(scores - jnp.max(scores, axis=1, keepdims=True))
            total = jnp.sum(e, axis=1, keepdims=True)
            num = jnp.dot(e.astype(bf16), values, preferred_element_type=f32)
            attended = jnp.where(here, num / total, attended)
        mixture = (
            mine[...] + jnp.dot(attended.astype(bf16), ow[...], preferred_element_type=f32)
        ).astype(bf16)
        picked = jnp.dot(sel[...], mixture, preferred_element_type=f32).astype(bf16)

        row = lax.broadcasted_iota(jnp.int32, (stride, 1), 0)
        second_half = ((row + 3) // 4) % 2 == 0
        y_ok = ((row > 0) | (pos_ref[1] > 0)) & ((row < by + 1) | (pos_ref[1] < ny - 1))
        zl = lax.broadcasted_iota(jnp.int32, (1, wide), 1)
        z_ok = ((zl >= chan) | (pos_ref[2] > 0)) & ((zl < (bz + 1) * chan) | (pos_ref[2] < nz - 1))
        ok = y_ok & z_ok
        x_lo, x_hi = pos_ref[0] > 0, pos_ref[0] < nx - 1
        if padded > wide:
            grid[:, wide:] = jnp.zeros((tall, padded - wide), f32)
        step = len(zs) * stride
        for xi, (first, many, _, _, a) in enumerate(xs):
            raised = jnp.dot(
                picked[xi * step : (xi + 1) * step], upx_ref[a], preferred_element_type=f32
            )
            parts = []
            for zi, (_, _, (l0, l1)) in enumerate(zs):
                block = raised[zi * stride : (zi + 1) * stride]
                half = block.shape[1] // 2
                chosen = jnp.where(second_half, block[:, half:], block[:, :half])
                parts.append(chosen[:, l0:l1])
            upward = jnp.concatenate(parts, axis=1)
            for x in range(first, first + many):
                good = ok
                if x == 0:
                    good = ok & x_lo
                if x == bx + 1:
                    good = ok & x_hi
                cells = enc[x * stride : (x + 1) * stride, :].astype(f32)
                grid[x * stride : (x + 1) * stride, :wide] = jnp.where(good, cells + upward, 0.0)
        outs = banded_conv(grid, w, sums, blocks, low, stride, chan)
        final = jnp.concatenate(outs, axis=1)[:, : bz * chan].astype(bf16)
        for x in range(bx):
            out[x] = final[x * stride : x * stride + by].reshape(by, bz, chan)

    return call(
        attend,
        jax.ShapeDtypeStruct(shape, bf16),
        scratch=[
            pltpu.VMEM((every, width), f32),
            pltpu.VMEM((asked, width), f32),
            pltpu.VMEM((asked, width), f32),
            pltpu.VMEM((tall, padded), f32),
            pltpu.VMEM((3, low + 8, OUT_Z * chan), f32),
        ],
        in_smem=1,
        total=10,
    )(
        pos, gathered, gain, q_weight, kv_weight, out_weight, upx, jnp.asarray(pick, bf16), encoded, weights
    )


def on_device(volume, conv_in, conv_out, norm_gain, q_weight, kv_weight, out_weight, up_weight):
    shape = volume.shape
    bx, by, bz, chan = shape
    counts = tuple(lax.axis_size(axis) for axis in AXES)
    pos = jnp.stack([lax.axis_index(axis) for axis in AXES]).astype(jnp.int32)
    first_w, second_w, upx = band_weights(conv_in, conv_out, up_weight, chan)

    z_below, z_above = exchange(
        volume[:, :, :2].reshape(bx * by, 2 * chan),
        volume[:, :, bz - 2 :].reshape(bx * by, 2 * chan),
        "gz",
    )
    rows, y_low, y_high = pack_rows(volume, z_below, z_above)
    y_below, y_above = exchange(y_low, y_high, "gy")
    yfaces = [y_below] if counts[1] <= 2 else [y_below, y_above]
    x_below, x_above = exchange(
        jnp.concatenate([rows[: 2 * by]] + [face[:4] for face in yfaces], axis=0),
        jnp.concatenate([rows[(bx - 2) * by :]] + [face[(bx - 2) * 2 :] for face in yfaces], axis=0),
        "gx",
    )
    encoded, tokens = encode(pos, rows, yfaces, x_below, x_above, first_w, shape, counts)

    devices = counts[0] * counts[1] * counts[2]
    copies = jnp.broadcast_to(tokens[None], (devices,) + tokens.shape)
    gathered = lax.all_to_all(copies, AXES, 0, 0, tiled=True).reshape(-1, tokens.shape[1])
    return attend_and_join(
        pos, gathered, norm_gain[None], q_weight, kv_weight, out_weight, upx, encoded, second_w, shape, counts
    )


def solution(mesh):
    placed = (P("gx", "gy", "gz", None), P(), P(), P(), P(), P(), P(), P())
    return jax.shard_map(
        on_device, mesh=mesh, in_specs=placed, out_specs=P("gx", "gy", "gz", None), check_vma=False
    )
```

```python
import numpy as np

import jax
import jax.numpy as jnp
from jax import lax
from jax.experimental import pallas as pl
from jax.experimental.pallas import tpu as pltpu
from jax.sharding import PartitionSpec as P

HEADS = 8
AXES = ("gx", "gy", "gz")
OUT_Z = 6
IN_Z = 8

f32 = jnp.float32
bf16 = jnp.bfloat16


def paired(count):
    return count > 2 and count % 2 == 0


def sends(low, high, index, count):
    if count <= 2:
        return [jnp.where(index == 0, high, low)]
    if not paired(count):
        return [high, low]
    even = index % 2 == 0
    return [jnp.where(even, high, low), jnp.where(even, low, high)]


def exchange(faces, axis):
    count = lax.axis_size(axis)
    if count == 1:
        return list(faces)
    if count == 2:
        return [lax.ppermute(faces[0], axis, [(0, 1), (1, 0)])]
    if not paired(count):
        up = [(i, (i + 1) % count) for i in range(count)]
        return [
            lax.ppermute(faces[0], axis, up),
            lax.ppermute(faces[1], axis, [(j, i) for i, j in up]),
        ]
    return [
        lax.ppermute(faces[0], axis, [(i, i ^ 1) for i in range(count)]),
        lax.ppermute(
            faces[1],
            axis,
            [(i, (i + 1) % count if i % 2 else (i - 1) % count) for i in range(count)],
        ),
    ]


def received(got, index, count):
    if len(got) == 1:
        return got[0], got[0]
    if not paired(count):
        return got[0], got[1]
    even = index % 2 == 0
    return jnp.where(even, got[1], got[0]), jnp.where(even, got[0], got[1])


def call(body, outs, scratch=(), operands=0, limit=16 << 20):
    return pl.pallas_call(
        body,
        out_shape=outs,
        in_specs=[pl.BlockSpec(memory_space=pltpu.VMEM)] * operands,
        scratch_shapes=list(scratch),
        compiler_params=pltpu.CompilerParams(vmem_limit_bytes=limit),
        name=body.__name__,
    )


def band_weights(kernel_in, kernel_out, up_weight, chan):
    width = up_weight.shape[0]

    def spread_weights(kin, kout, up, first, second, upx):
        for source, target in ((kin, first), (kout, second)):
            target[...] = jnp.zeros(target.shape, target.dtype)
            for tap in range(9):
                block = source[tap]
                for z in range(OUT_Z):
                    target[tap, z * chan : (z + 3) * chan, z * chan : (z + 1) * chan] = block
        for a in range(2):
            pieces = []
            for b in range(2):
                for c in range(2):
                    start = (a * 4 + b * 2 + c) * chan
                    pieces += [up[:, start : start + chan]] * 4
            upx[a] = jnp.concatenate(pieces, axis=1)

    banded = jax.ShapeDtypeStruct((9, IN_Z * chan, OUT_Z * chan), bf16)
    return call(
        spread_weights,
        (banded, banded, jax.ShapeDtypeStruct((2, width, 16 * chan), bf16)),
        operands=3,
    )(
        kernel_in.reshape(9, 3 * chan, chan),
        kernel_out.reshape(9, 3 * chan, chan),
        up_weight,
    )


def pack_rows(volume):
    bx, by, bz, chan = volume.shape

    def pack(vol, rows):
        rows[...] = vol[...].reshape(bx * by, bz * chan)

    return call(pack, jax.ShapeDtypeStruct((bx * by, bz * chan), bf16), operands=1)(volume)


def y_faces(rows, zgot, shape, counts):
    bx, by, bz, chan = shape
    lanes = (bz + 4) * chan
    many = 1 if counts[1] <= 2 else 2
    parts = len(zgot)

    def y_face(own, *refs):
        zm, zp = received([r[...].astype(f32) for r in refs[:parts]], lax.axis_index("gz"), counts[2])
        full = jnp.concatenate([zm, own[...].astype(f32), zp], axis=1)
        low, high = [], []
        for x in range(bx):
            low.append(full[x * by : x * by + 2])
            high.append(full[(x + 1) * by - 2 : (x + 1) * by])
        faces = sends(
            jnp.concatenate(low, axis=0), jnp.concatenate(high, axis=0), lax.axis_index("gy"), counts[1]
        )
        for ref, face in zip(refs[parts:], faces):
            ref[...] = face.astype(bf16)

    face = jax.ShapeDtypeStruct((bx * 2, lanes), bf16)
    return call(y_face, (face,) * many, operands=1 + parts)(rows, *zgot)


def x_faces(rows, zgot, ygot, shape, counts):
    bx, by, bz, chan = shape
    lanes = (bz + 4) * chan
    zparts, yparts = len(zgot), len(ygot)
    many = 1 if counts[0] <= 2 else 2
    tall = 2 * by + 4 * yparts

    def x_face(own, *refs):
        zrefs, yrefs, outs = refs[:zparts], refs[zparts : zparts + yparts], refs[zparts + yparts :]
        index = lax.axis_index("gz")

        def face(first):
            at = slice(first * by, (first + 2) * by)
            zm, zp = received([r[at, :].astype(f32) for r in zrefs], index, counts[2])
            body = jnp.concatenate([zm, own[at, :].astype(f32), zp], axis=1)
            edges = [r[...].astype(f32)[2 * first : 2 * first + 4] for r in yrefs]
            return jnp.concatenate([body] + edges, axis=0)

        for ref, value in zip(outs, sends(face(0), face(bx - 2), lax.axis_index("gx"), counts[0])):
            ref[...] = value.astype(bf16)

    face = jax.ShapeDtypeStruct((tall, lanes), bf16)
    return call(x_face, (face,) * many, operands=1 + zparts + yparts)(rows, *zgot, *ygot)


def banded_conv(source, weights, sums, blocks, rows, stride, chan):
    outs = []
    for block in range(blocks):
        start = block * OUT_Z * chan
        for dy in range(3):
            total = None
            for dx in range(3):
                piece = source[dx * stride : dx * stride + rows, start : start + IN_Z * chan]
                part = jnp.dot(
                    piece.astype(bf16), weights[dx * 3 + dy], preferred_element_type=f32
                )
                total = part if total is None else total + part
            sums[dy, :rows, :] = total
        outs.append(sums[0, 0:rows, :] + sums[1, 1 : rows + 1, :] + sums[2, 2 : rows + 2, :])
    return outs


def encode(rows, zgot, ygot, xgot, weights, shape, counts):
    bx, by, bz, chan = shape
    nx, ny, nz = counts
    lanes = (bz + 4) * chan
    stride = by + 8
    tall = (bx + 2) * stride
    blocks = (bz + 2) // OUT_Z
    ti, tj, tk = bx // 8, by // 8, bz // 8
    tokens = ti * tj * tk
    width = 8 * chan
    zparts, yparts, xparts = len(zgot), len(ygot), len(xgot)
    devices = nx * ny * nz

    def encode_rows(own, *refs):
        zrefs, refs = refs[:zparts], refs[zparts:]
        yrefs, refs = refs[:yparts], refs[yparts:]
        xrefs, refs = refs[:xparts], refs[xparts:]
        w, enc, tok_copies, grid, sums, plane_sum = refs
        ix, iy, iz = (lax.axis_index(axis) for axis in AXES)
        lane = lax.broadcasted_iota(jnp.int32, (1, lanes), 1)
        z_ok = ((lane >= 2 * chan) | (iz > 0)) & ((lane < (bz + 2) * chan) | (iz < nz - 1))
        y_lo, y_hi = iy > 0, iy < ny - 1
        x_lo, x_hi = ix > 0, ix < nx - 1

        def put(row, value, ok=None):
            good = z_ok if ok is None else z_ok & ok
            grid[row : row + value.shape[0], :] = jnp.where(good, value, 0.0)

        ym, yp = received([r[...].astype(f32) for r in yrefs], iy, ny)
        for p in range(bx):
            base = (p + 2) * stride
            at = slice(p * by, (p + 1) * by)
            zm, zp = received([r[at, :].astype(f32) for r in zrefs], iz, nz)
            put(base + 2, jnp.concatenate([zm, own[at, :].astype(f32), zp], axis=1))
            put(base, ym[2 * p : 2 * p + 2], y_lo)
            put(base + by + 2, yp[2 * p : 2 * p + 2], y_hi)
        xm, xp = received([r[...].astype(f32) for r in xrefs], ix, nx)
        for face, first, ok in ((xm, 0, x_lo), (xp, bx + 2, x_hi)):
            for q in range(2):
                base = (first + q) * stride
                put(base + 2, face[q * by : (q + 1) * by], ok)
                at = 2 * by + 2 * q
                low = received([face[at + 4 * i : at + 4 * i + 2] for i in range(yparts)], iy, ny)
                put(base, low[0], ok & y_lo)
                put(base + by + 2, low[1], ok & y_hi)
        outs = banded_conv(grid, w, sums, blocks, tall, stride, chan)
        encoded = jnp.maximum(jnp.concatenate(outs, axis=1), 0.0).astype(bf16)
        enc[...] = encoded
        cells = encoded.astype(f32)
        rows_of = {}
        for i in range(ti):
            features = {}
            for a in range(2):
                x0 = 1 + 8 * i + 4 * a
                acc = cells[x0 * stride : (x0 + 1) * stride]
                for q in range(1, 4):
                    acc = acc + cells[(x0 + q) * stride : (x0 + q + 1) * stride]
                for g in range(2 * tk):
                    at = (1 + 4 * g) * chan
                    plane_sum[g] = acc[:, at : at + 4 * chan]
                for b in range(2):
                    for g in range(2 * tk):
                        part = None
                        for q in range(4):
                            line = plane_sum[g, pl.ds(1 + 4 * b + q, tj, stride=8), :]
                            part = line if part is None else part + line
                        s = part[:, :chan]
                        for q in range(1, 4):
                            s = s + part[:, q * chan : (q + 1) * chan]
                        features[a, b, g] = s * (1.0 / 64.0)
            for k in range(tk):
                rows_of[i, k] = jnp.concatenate(
                    [features[a, b, 2 * k + c] for a in range(2) for b in range(2) for c in range(2)],
                    axis=1,
                )
        own_tokens = jnp.concatenate([rows_of[i, k] for i in range(ti) for k in range(tk)], axis=0)
        for device in range(devices):
            tok_copies[device] = own_tokens

    return call(
        encode_rows,
        (
            jax.ShapeDtypeStruct((tall, (bz + 2) * chan), bf16),
            jax.ShapeDtypeStruct((devices, tokens, width), f32),
        ),
        scratch=[
            pltpu.VMEM(((bx + 4) * stride, lanes), f32),
            pltpu.VMEM((3, tall + 8, OUT_Z * chan), f32),
            pltpu.VMEM((2 * tk, stride, 4 * chan), f32),
        ],
        operands=2 + zparts + yparts + xparts,
    )(rows, *zgot, *ygot, *xgot, weights)


def sub_blocks(extent):
    out = [(0, 1, -1, extent // 8 - 1, 1)]
    for s in range(extent // 4):
        out.append((1 + 4 * s, 4, 0, s // 2, s % 2))
    out.append((extent + 1, 1, 1, 0, 0))
    return out


def attend_and_join(
    gathered, gain, q_weight, kv_weight, out_weight, upx, encoded, weights, shape, counts
):
    bx, by, bz, chan = shape
    nx, ny, nz = counts
    stride = by + 8
    tall, low = (bx + 2) * stride, bx * stride
    ti, tj, tk = bx // 8, by // 8, bz // 8
    tokens = ti * tj * tk
    width = 8 * chan
    every = gathered.shape[0] * tokens
    asked = 27 * tokens
    head_size = width // HEADS
    wide = (bz + 2) * chan
    blocks = -(-bz // OUT_Z)
    padded = (blocks * OUT_Z + 2) * chan

    xs = sub_blocks(bx)
    zs = [(-1, tk - 1, (7 * chan, 8 * chan))]
    zs += [(0, k, (0, 8 * chan)) for k in range(tk)]
    zs += [(1, 0, (0, chan))]
    pick = np.zeros((len(xs) * len(zs) * stride, asked), np.float32)
    for xi, (_, _, dx, i, _) in enumerate(xs):
        for zi, (dz, k, _) in enumerate(zs):
            for first, many, dy, j, _ in sub_blocks(by):
                near = ((dx + 1) * 3 + dy + 1) * 3 + dz + 1
                row = (xi * len(zs) + zi) * stride + first
                pick[row : row + many, near * tokens + (i * tk + k) * tj + j] = 1.0

    def attend(
        g, gain_ref, qw, kvw, ow, upx_ref, sel, enc, w, out, normed_all, mine, mine_n, grid, sums
    ):
        ix, iy, iz = (lax.axis_index(axis) for axis in AXES)
        t = g[...].reshape(every, width)
        center = t - jnp.mean(t, axis=1, keepdims=True)
        spread = jnp.mean(center * center, axis=1, keepdims=True)
        normed = (center * lax.rsqrt(spread + 1e-05) * gain_ref[...]).astype(bf16)
        normed_all[...] = normed.astype(f32)
        kv = jnp.dot(normed, kvw[...], preferred_element_type=f32).astype(bf16)
        keys, values = kv[:, :width], kv[:, width:]
        near = 0
        for dx in (-1, 0, 1):
            x = jnp.clip(ix + dx, 0, nx - 1)
            for dy in (-1, 0, 1):
                y = jnp.clip(iy + dy, 0, ny - 1)
                for dz in (-1, 0, 1):
                    z = jnp.clip(iz + dz, 0, nz - 1)
                    at = pl.multiple_of(((x * ny + y) * nz + z) * tokens, 8)
                    mine[near * tokens : (near + 1) * tokens, :] = g[(x * ny + y) * nz + z]
                    mine_n[near * tokens : (near + 1) * tokens, :] = normed_all[pl.ds(at, tokens), :]
                    near += 1
        q = jnp.dot(mine_n[...].astype(bf16), qw[...], preferred_element_type=f32).astype(bf16)
        lane = lax.broadcasted_iota(jnp.int32, (1, width), 1) // head_size
        attended = jnp.zeros((asked, width), f32)
        for h in range(HEADS):
            here = lane == h
            q_h = jnp.where(here, q, jnp.zeros_like(q))
            scores = (
                lax.dot_general(q_h, keys, (((1,), (1,)), ((), ())), preferred_element_type=f32)
                * head_size ** (-0.5)
            )
            e = jnp.exp(scores - jnp.max(scores, axis=1, keepdims=True))
            total = jnp.sum(e, axis=1, keepdims=True)
            num = jnp.dot(e.astype(bf16), values, preferred_element_type=f32)
            attended = jnp.where(here, num / total, attended)
        mixture = (
            mine[...] + jnp.dot(attended.astype(bf16), ow[...], preferred_element_type=f32)
        ).astype(bf16)
        picked = jnp.dot(sel[...], mixture, preferred_element_type=f32).astype(bf16)

        row = lax.broadcasted_iota(jnp.int32, (stride, 1), 0)
        second_half = ((row + 3) // 4) % 2 == 0
        y_ok = ((row > 0) | (iy > 0)) & ((row < by + 1) | (iy < ny - 1))
        zl = lax.broadcasted_iota(jnp.int32, (1, wide), 1)
        z_ok = ((zl >= chan) | (iz > 0)) & ((zl < (bz + 1) * chan) | (iz < nz - 1))
        ok = y_ok & z_ok
        x_lo, x_hi = ix > 0, ix < nx - 1
        if padded > wide:
            grid[:, wide:] = jnp.zeros((tall, padded - wide), f32)
        step = len(zs) * stride
        for xi, (first, many, _, _, a) in enumerate(xs):
            raised = jnp.dot(
                picked[xi * step : (xi + 1) * step], upx_ref[a], preferred_element_type=f32
            )
            parts = []
            for zi, (_, _, (l0, l1)) in enumerate(zs):
                block = raised[zi * stride : (zi + 1) * stride]
                half = block.shape[1] // 2
                chosen = jnp.where(second_half, block[:, half:], block[:, :half])
                parts.append(chosen[:, l0:l1])
            upward = jnp.concatenate(parts, axis=1)
            for x in range(first, first + many):
                good = ok
                if x == 0:
                    good = ok & x_lo
                if x == bx + 1:
                    good = ok & x_hi
                cells = enc[x * stride : (x + 1) * stride, :].astype(f32)
                grid[x * stride : (x + 1) * stride, :wide] = jnp.where(good, cells + upward, 0.0)
        outs = banded_conv(grid, w, sums, blocks, low, stride, chan)
        final = jnp.concatenate(outs, axis=1)[:, : bz * chan].astype(bf16)
        for x in range(bx):
            out[x] = final[x * stride : x * stride + by].reshape(by, bz, chan)

    return call(
        attend,
        jax.ShapeDtypeStruct(shape, bf16),
        scratch=[
            pltpu.VMEM((every, width), f32),
            pltpu.VMEM((asked, width), f32),
            pltpu.VMEM((asked, width), f32),
            pltpu.VMEM((tall, padded), f32),
            pltpu.VMEM((3, low + 8, OUT_Z * chan), f32),
        ],
        operands=9,
        limit=min(60, 18 + 24 * every * asked // (1 << 20)) << 20,
    )(
        gathered, gain, q_weight, kv_weight, out_weight, upx, jnp.asarray(pick, bf16), encoded, weights
    )


def on_device(volume, conv_in, conv_out, norm_gain, q_weight, kv_weight, out_weight, up_weight):
    shape = volume.shape
    bx, by, bz, chan = shape
    counts = tuple(lax.axis_size(axis) for axis in AXES)
    first_w, second_w, upx = band_weights(conv_in, conv_out, up_weight, chan)
    zgot = exchange(
        sends(
            volume[:, :, :2].reshape(bx * by, 2 * chan),
            volume[:, :, bz - 2 :].reshape(bx * by, 2 * chan),
            lax.axis_index("gz"),
            counts[2],
        ),
        "gz",
    )
    rows = pack_rows(volume)
    ygot = exchange(y_faces(rows, zgot, shape, counts), "gy")
    xgot = exchange(x_faces(rows, zgot, ygot, shape, counts), "gx")
    encoded, copies = encode(rows, zgot, ygot, xgot, first_w, shape, counts)
    gathered = lax.all_to_all(copies, AXES, 0, 0, tiled=True)
    return attend_and_join(
        gathered, norm_gain[None], q_weight, kv_weight, out_weight, upx, encoded, second_w, shape, counts
    )


def solution(mesh):
    placed = (P("gx", "gy", "gz", None), P(), P(), P(), P(), P(), P(), P())
    return jax.shard_map(
        on_device, mesh=mesh, in_specs=placed, out_specs=P("gx", "gy", "gz", None), check_vma=False
    )
```

```python
import numpy as np

import jax
import jax.numpy as jnp
from jax import lax
from jax.experimental import pallas as pl
from jax.experimental.pallas import tpu as pltpu
from jax.sharding import PartitionSpec as P

HEADS = 8
AXES = ("gx", "gy", "gz")
OUT_Z = 6
IN_Z = 8

f32 = jnp.float32
bf16 = jnp.bfloat16


def paired(count):
    return count > 2 and count % 2 == 0


def sends(low, high, index, count):
    if count <= 2:
        return [jnp.where(index == 0, high, low)]
    if not paired(count):
        return [high, low]
    even = index % 2 == 0
    return [jnp.where(even, high, low), jnp.where(even, low, high)]


def exchange(faces, axis):
    count = lax.axis_size(axis)
    if count == 1:
        return list(faces)
    if count == 2:
        return [lax.ppermute(faces[0], axis, [(0, 1), (1, 0)])]
    if not paired(count):
        up = [(i, (i + 1) % count) for i in range(count)]
        return [
            lax.ppermute(faces[0], axis, up),
            lax.ppermute(faces[1], axis, [(j, i) for i, j in up]),
        ]
    return [
        lax.ppermute(faces[0], axis, [(i, i ^ 1) for i in range(count)]),
        lax.ppermute(
            faces[1],
            axis,
            [(i, (i + 1) % count if i % 2 else (i - 1) % count) for i in range(count)],
        ),
    ]


def received(got, index, count):
    if len(got) == 1:
        return got[0], got[0]
    if not paired(count):
        return got[0], got[1]
    even = index % 2 == 0
    return jnp.where(even, got[1], got[0]), jnp.where(even, got[0], got[1])


def call(body, outs, scratch=(), operands=0, limit=16 << 20):
    return pl.pallas_call(
        body,
        out_shape=outs,
        in_specs=[pl.BlockSpec(memory_space=pltpu.VMEM)] * operands,
        scratch_shapes=list(scratch),
        compiler_params=pltpu.CompilerParams(vmem_limit_bytes=limit),
        name=body.__name__,
    )


def band_weights(kernel_in, kernel_out, up_weight, chan):
    width = up_weight.shape[0]

    def spread_weights(kin, kout, up, first, second, upx):
        for source, target in ((kin, first), (kout, second)):
            target[...] = jnp.zeros(target.shape, target.dtype)
            for tap in range(9):
                block = source[tap]
                for z in range(OUT_Z):
                    target[tap, z * chan : (z + 3) * chan, z * chan : (z + 1) * chan] = block
        for a in range(2):
            pieces = []
            for b in range(2):
                for c in range(2):
                    start = (a * 4 + b * 2 + c) * chan
                    pieces += [up[:, start : start + chan]] * 4
            upx[a] = jnp.concatenate(pieces, axis=1)

    banded = jax.ShapeDtypeStruct((9, IN_Z * chan, OUT_Z * chan), bf16)
    return call(
        spread_weights,
        (banded, banded, jax.ShapeDtypeStruct((2, width, 16 * chan), bf16)),
        operands=3,
    )(
        kernel_in.reshape(9, 3 * chan, chan),
        kernel_out.reshape(9, 3 * chan, chan),
        up_weight,
    )


def pack_rows(volume, counts):
    bx, by, bz, chan = volume.shape
    many = 1 if counts[2] <= 2 else 2
    half = bx * by // 2

    def pack(vol, rows, *refs):
        outs, (here, arrived) = refs[:many], refs[many:]
        copies = [pltpu.make_async_copy(vol.at[x], here.at[x], arrived.at[x]) for x in range(bx)]
        for copy in copies:
            copy.start()
        for x in range(bx):
            copies[x].wait()
            rows[x * by : (x + 1) * by, :] = here[x].reshape(by, bz * chan)

        def beside(start):
            return jnp.concatenate(
                [rows[:half, start : start + 2 * chan], rows[half:, start : start + 2 * chan]], axis=1
            )

        faces = sends(beside(0), beside((bz - 2) * chan), lax.axis_index("gz"), counts[2])
        for ref, face in zip(outs, faces):
            ref[...] = face

    return pl.pallas_call(
        pack,
        out_shape=(jax.ShapeDtypeStruct((bx * by, bz * chan), bf16),)
        + (jax.ShapeDtypeStruct((half, 4 * chan), bf16),) * many,
        in_specs=[pl.BlockSpec(memory_space=pltpu.HBM)],
        scratch_shapes=[pltpu.VMEM(volume.shape, bf16), pltpu.SemaphoreType.DMA((bx,))],
        compiler_params=pltpu.CompilerParams(vmem_limit_bytes=16 << 20),
        name="pack",
    )(pltpu.with_memory_space_constraint(volume, pltpu.HBM))


def full_rows(own, zrefs, plane, shape, count):
    bx, by, bz, chan = shape
    side, at = divmod(plane, bx // 2)
    parts = [
        r[at * by : (at + 1) * by, side * 2 * chan : (side + 1) * 2 * chan].astype(f32) for r in zrefs
    ]
    zm, zp = received(parts, lax.axis_index("gz"), count)
    return jnp.concatenate([zm, own[plane * by : (plane + 1) * by, :].astype(f32), zp], axis=1)


def y_faces(rows, zgot, shape, counts):
    bx, by, bz, chan = shape
    lanes = (bz + 4) * chan
    many = 1 if counts[1] <= 2 else 2
    parts = len(zgot)

    def y_face(own, *refs):
        low, high = [], []
        for x in range(bx):
            full = full_rows(own, refs[:parts], x, shape, counts[2])
            low.append(full[:2])
            high.append(full[by - 2 :])
        faces = sends(
            jnp.concatenate(low, axis=0), jnp.concatenate(high, axis=0), lax.axis_index("gy"), counts[1]
        )
        for ref, face in zip(refs[parts:], faces):
            ref[...] = face.astype(bf16)

    face = jax.ShapeDtypeStruct((bx * 2, lanes), bf16)
    return call(y_face, (face,) * many, operands=1 + parts)(rows, *zgot)


def x_faces(rows, zgot, ygot, shape, counts):
    bx, by, bz, chan = shape
    lanes = (bz + 4) * chan
    zparts, yparts = len(zgot), len(ygot)
    many = 1 if counts[0] <= 2 else 2
    tall = 2 * by + 4 * yparts

    def x_face(own, *refs):
        zrefs, yrefs, outs = refs[:zparts], refs[zparts : zparts + yparts], refs[zparts + yparts :]

        def face(first):
            body = [full_rows(own, zrefs, first + q, shape, counts[2]) for q in range(2)]
            edges = [r[...].astype(f32)[2 * first : 2 * first + 4] for r in yrefs]
            return jnp.concatenate(body + edges, axis=0)

        for ref, value in zip(outs, sends(face(0), face(bx - 2), lax.axis_index("gx"), counts[0])):
            ref[...] = value.astype(bf16)

    face = jax.ShapeDtypeStruct((tall, lanes), bf16)
    return call(x_face, (face,) * many, operands=1 + zparts + yparts)(rows, *zgot, *ygot)


def banded_conv(source, weights, sums, blocks, starts, rows, stride, chan):
    outs = []
    tall = rows * len(starts)
    for block in range(blocks):
        lane = block * OUT_Z * chan
        for dy in range(3):
            total = None
            for dx in range(3):
                pieces = [
                    source[at + dx * stride : at + dx * stride + rows, lane : lane + IN_Z * chan]
                    for at in starts
                ]
                piece = pieces[0] if len(pieces) == 1 else jnp.concatenate(pieces, axis=0)
                part = jnp.dot(
                    piece.astype(bf16), weights[dx * 3 + dy], preferred_element_type=f32
                )
                total = part if total is None else total + part
            sums[dy, :tall, :] = total
        outs.append(sums[0, 0:tall, :] + sums[1, 1 : tall + 1, :] + sums[2, 2 : tall + 2, :])
    return outs


def put_plane(grid, row, own, zrefs, yrefs, plane, shape, counts):
    bx, by, bz, chan = shape
    nx, ny, nz = counts
    iy, iz = lax.axis_index("gy"), lax.axis_index("gz")
    lane = lax.broadcasted_iota(jnp.int32, (1, (bz + 4) * chan), 1)
    z_ok = ((lane >= 2 * chan) | (iz > 0)) & ((lane < (bz + 2) * chan) | (iz < nz - 1))
    full = full_rows(own, zrefs, plane, shape, nz)
    grid[row + 2 : row + 2 + by, :] = jnp.where(z_ok, full, 0.0)
    ym, yp = received(
        [r[...].astype(f32)[2 * plane : 2 * plane + 2] for r in yrefs], iy, ny
    )
    grid[row : row + 2, :] = jnp.where(z_ok & (iy > 0), ym, 0.0)
    grid[row + by + 2 : row + by + 4, :] = jnp.where(z_ok & (iy < ny - 1), yp, 0.0)


def relu_rows(outs):
    return jnp.maximum(jnp.concatenate(outs, axis=1), 0.0).astype(bf16)


def encode_inner(rows, zgot, ygot, weights, shape, counts):
    bx, by, bz, chan = shape
    lanes = (bz + 4) * chan
    stride = by + 8
    tall = (bx - 2) * stride
    groups = bx // 4
    zparts, yparts = len(zgot), len(ygot)

    def encode_middle(own, *refs):
        zrefs, refs = refs[:zparts], refs[zparts:]
        yrefs, (w, enc, partial, grid, sums) = refs[:yparts], refs[yparts:]
        for p in range(bx):
            put_plane(grid, p * stride, own, zrefs, yrefs, p, shape, counts)
        outs = banded_conv(grid, w, sums, (bz + 2) // OUT_Z, [0], tall, stride, chan)
        encoded = relu_rows(outs)
        enc[...] = encoded
        cells = encoded.astype(f32)
        for group in range(groups):
            total = None
            for x in range(max(1, 4 * group), min(bx - 1, 4 * group + 4)):
                plane = cells[(x - 1) * stride : x * stride]
                total = plane if total is None else total + plane
            partial[group * stride : (group + 1) * stride, :] = total

    return call(
        encode_middle,
        (
            jax.ShapeDtypeStruct((tall, (bz + 2) * chan), bf16),
            jax.ShapeDtypeStruct((groups * stride, (bz + 2) * chan), f32),
        ),
        scratch=[
            pltpu.VMEM((bx * stride, lanes), f32),
            pltpu.VMEM((3, tall + 8, OUT_Z * chan), f32),
        ],
        operands=2 + zparts + yparts,
    )(rows, *zgot, *ygot, weights)


def encode_outer(rows, zgot, ygot, xgot, weights, partial, shape, counts):
    bx, by, bz, chan = shape
    nx, ny, nz = counts
    lanes = (bz + 4) * chan
    stride = by + 8
    tall = 4 * stride
    groups = bx // 4
    ti, tj, tk = bx // 8, by // 8, bz // 8
    tokens = ti * tj * tk
    width = 8 * chan
    zparts, yparts, xparts = len(zgot), len(ygot), len(xgot)
    devices = nx * ny * nz

    def encode_ends(own, *refs):
        zrefs, refs = refs[:zparts], refs[zparts:]
        yrefs, refs = refs[:yparts], refs[yparts:]
        xrefs, refs = refs[:xparts], refs[xparts:]
        w, part_ref, enc, tok_copies, grid, sums, plane_sum = refs
        ix, iy, iz = (lax.axis_index(axis) for axis in AXES)
        lane = lax.broadcasted_iota(jnp.int32, (1, lanes), 1)
        z_ok = ((lane >= 2 * chan) | (iz > 0)) & ((lane < (bz + 2) * chan) | (iz < nz - 1))
        for slot, plane in ((2, 0), (3, 1), (4, bx - 2), (5, bx - 1)):
            put_plane(grid, slot * stride, own, zrefs, yrefs, plane, shape, counts)
        xm, xp = received([r[...].astype(f32) for r in xrefs], ix, nx)
        for face, first, ok in ((xm, 0, ix > 0), (xp, 6, ix < nx - 1)):
            good = z_ok & ok
            for q in range(2):
                base = (first + q) * stride
                grid[base + 2 : base + 2 + by, :] = jnp.where(good, face[q * by : (q + 1) * by], 0.0)
                at = 2 * by + 2 * q
                ym, yp = received([face[at + 4 * i : at + 4 * i + 2] for i in range(yparts)], iy, ny)
                grid[base : base + 2, :] = jnp.where(good & (iy > 0), ym, 0.0)
                grid[base + by + 2 : base + by + 4, :] = jnp.where(good & (iy < ny - 1), yp, 0.0)
        outs = banded_conv(
            grid, w, sums, (bz + 2) // OUT_Z, [0, 4 * stride], 2 * stride, stride, chan
        )
        encoded = relu_rows(outs)
        enc[...] = encoded
        first_plane = encoded[stride : 2 * stride].astype(f32)
        last_plane = encoded[2 * stride : 3 * stride].astype(f32)
        rows_of = {}
        for i in range(ti):
            features = {}
            for a in range(2):
                group = 2 * i + a
                acc = part_ref[group * stride : (group + 1) * stride, :]
                if group == 0:
                    acc = acc + first_plane
                if group == groups - 1:
                    acc = acc + last_plane
                for g in range(2 * tk):
                    at = (1 + 4 * g) * chan
                    plane_sum[g] = acc[:, at : at + 4 * chan]
                for b in range(2):
                    for g in range(2 * tk):
                        part = None
                        for q in range(4):
                            line = plane_sum[g, pl.ds(1 + 4 * b + q, tj, stride=8), :]
                            part = line if part is None else part + line
                        s = part[:, :chan]
                        for q in range(1, 4):
                            s = s + part[:, q * chan : (q + 1) * chan]
                        features[a, b, g] = s * (1.0 / 64.0)
            for k in range(tk):
                rows_of[i, k] = jnp.concatenate(
                    [features[a, b, 2 * k + c] for a in range(2) for b in range(2) for c in range(2)],
                    axis=1,
                )
        own_tokens = jnp.concatenate([rows_of[i, k] for i in range(ti) for k in range(tk)], axis=0)
        for device in range(devices):
            tok_copies[device] = own_tokens

    return call(
        encode_ends,
        (
            jax.ShapeDtypeStruct((tall, (bz + 2) * chan), bf16),
            jax.ShapeDtypeStruct((devices, tokens, width), f32),
        ),
        scratch=[
            pltpu.VMEM((8 * stride, lanes), f32),
            pltpu.VMEM((3, tall + 8, OUT_Z * chan), f32),
            pltpu.VMEM((2 * tk, stride, 4 * chan), f32),
        ],
        operands=3 + zparts + yparts + xparts,
        limit=(16 if devices <= 64 else 32) << 20,
    )(rows, *zgot, *ygot, *xgot, weights, partial)


def sub_blocks(extent):
    out = [(0, 1, -1, extent // 8 - 1, 1)]
    for s in range(extent // 4):
        out.append((1 + 4 * s, 4, 0, s // 2, s % 2))
    out.append((extent + 1, 1, 1, 0, 0))
    return out


def attend_and_join(
    gathered, gain, q_weight, kv_weight, out_weight, upx, inner, outer, weights, shape, counts
):
    bx, by, bz, chan = shape
    nx, ny, nz = counts
    stride = by + 8
    tall, low = (bx + 2) * stride, bx * stride
    ti, tj, tk = bx // 8, by // 8, bz // 8
    tokens = ti * tj * tk
    width = 8 * chan
    every = gathered.shape[0] * tokens
    runs, place = [], {}
    for dx in (-1, 0, 1):
        for dy in (-1, 0, 1):
            for dz in (-1, 0, 1):
                for i in {-1: [ti - 1], 0: range(ti), 1: [0]}[dx]:
                    for k in {-1: [tk - 1], 0: range(tk), 1: [0]}[dz]:
                        j0, j1 = {-1: (tj - 1, tj), 0: (0, tj), 1: (0, 1)}[dy]
                        runs.append(((dx, dy, dz), (i * tk + k) * tj + j0, j1 - j0))
                        for j in range(j0, j1):
                            place[dx, dy, dz, i, j, k] = len(place)
    asked = -(-len(place) // 16) * 16
    head_size = width // HEADS
    wide = (bz + 2) * chan
    blocks = -(-bz // OUT_Z)
    padded = (blocks * OUT_Z + 2) * chan

    xs = sub_blocks(bx)
    zs = [(-1, tk - 1, (7 * chan, 8 * chan))]
    zs += [(0, k, (0, 8 * chan)) for k in range(tk)]
    zs += [(1, 0, (0, chan))]
    pick = np.zeros((len(xs) * len(zs) * stride, asked), np.float32)
    for xi, (_, _, dx, i, _) in enumerate(xs):
        for zi, (dz, k, _) in enumerate(zs):
            for first, many, dy, j, _ in sub_blocks(by):
                row = (xi * len(zs) + zi) * stride + first
                pick[row : row + many, place[dx, dy, dz, i, j, k]] = 1.0

    def attend(
        g, gain_ref, qw, kvw, ow, upx_ref, sel, enc_in, enc_out, w, out, normed_all, mine, mine_n, grid, sums
    ):
        ix, iy, iz = (lax.axis_index(axis) for axis in AXES)
        t = g[...].reshape(every, width)
        center = t - jnp.mean(t, axis=1, keepdims=True)
        spread = jnp.mean(center * center, axis=1, keepdims=True)
        normed = (center * lax.rsqrt(spread + 1e-05) * gain_ref[...]).astype(bf16)
        normed_all[...] = normed.astype(f32)
        kv = jnp.dot(normed, kvw[...], preferred_element_type=f32).astype(bf16)
        keys, values = kv[:, :width], kv[:, width:]
        blocks_of = {}
        row = 0
        for (dx, dy, dz), first, many in runs:
            if (dx, dy, dz) not in blocks_of:
                x = jnp.clip(ix + dx, 0, nx - 1)
                y = jnp.clip(iy + dy, 0, ny - 1)
                z = jnp.clip(iz + dz, 0, nz - 1)
                device = (x * ny + y) * nz + z
                at = pl.multiple_of(device * tokens, 8)
                blocks_of[dx, dy, dz] = g[device], normed_all[pl.ds(at, tokens), :]
            block, normed_block = blocks_of[dx, dy, dz]
            mine[row : row + many, :] = block[first : first + many]
            mine_n[row : row + many, :] = normed_block[first : first + many]
            row += many
        if asked > row:
            mine[row:, :] = jnp.zeros((asked - row, width), f32)
            mine_n[row:, :] = jnp.zeros((asked - row, width), f32)
        q = jnp.dot(mine_n[...].astype(bf16), qw[...], preferred_element_type=f32).astype(bf16)
        lane = lax.broadcasted_iota(jnp.int32, (1, width), 1) // head_size
        attended = jnp.zeros((asked, width), f32)
        for h in range(HEADS):
            here = lane == h
            q_h = jnp.where(here, q, jnp.zeros_like(q))
            scores = (
                lax.dot_general(q_h, keys, (((1,), (1,)), ((), ())), preferred_element_type=f32)
                * head_size ** (-0.5)
            )
            e = jnp.exp(scores - jnp.max(scores, axis=1, keepdims=True))
            total = jnp.sum(e, axis=1, keepdims=True)
            num = jnp.dot(e.astype(bf16), values, preferred_element_type=f32)
            attended = jnp.where(here, num / total, attended)
        mixture = (
            mine[...] + jnp.dot(attended.astype(bf16), ow[...], preferred_element_type=f32)
        ).astype(bf16)
        picked = jnp.dot(sel[...], mixture, preferred_element_type=f32).astype(bf16)

        row = lax.broadcasted_iota(jnp.int32, (stride, 1), 0)
        second_half = ((row + 3) // 4) % 2 == 0
        y_ok = ((row > 0) | (iy > 0)) & ((row < by + 1) | (iy < ny - 1))
        zl = lax.broadcasted_iota(jnp.int32, (1, wide), 1)
        z_ok = ((zl >= chan) | (iz > 0)) & ((zl < (bz + 1) * chan) | (iz < nz - 1))
        ok = y_ok & z_ok
        x_lo, x_hi = ix > 0, ix < nx - 1
        if padded > wide:
            grid[:, wide:] = jnp.zeros((tall, padded - wide), f32)
        step = len(zs) * stride
        for xi, (first, many, _, _, a) in enumerate(xs):
            raised = jnp.dot(
                picked[xi * step : (xi + 1) * step], upx_ref[a], preferred_element_type=f32
            )
            parts = []
            for zi, (_, _, (l0, l1)) in enumerate(zs):
                block = raised[zi * stride : (zi + 1) * stride]
                half = block.shape[1] // 2
                chosen = jnp.where(second_half, block[:, half:], block[:, :half])
                parts.append(chosen[:, l0:l1])
            upward = jnp.concatenate(parts, axis=1)
            for x in range(first, first + many):
                good = ok
                if x == 0:
                    good = ok & x_lo
                if x == bx + 1:
                    good = ok & x_hi
                ref, at = (enc_in, x - 2) if 2 <= x < bx else (enc_out, x if x < 2 else x - bx + 2)
                cells = ref[at * stride : (at + 1) * stride, :].astype(f32)
                grid[x * stride : (x + 1) * stride, :wide] = jnp.where(good, cells + upward, 0.0)
        outs = banded_conv(grid, w, sums, blocks, [0], low, stride, chan)
        final = jnp.concatenate(outs, axis=1)[:, : bz * chan].astype(bf16)
        for x in range(bx):
            out[x] = final[x * stride : x * stride + by].reshape(by, bz, chan)

    return call(
        attend,
        jax.ShapeDtypeStruct(shape, bf16),
        scratch=[
            pltpu.VMEM((every, width), f32),
            pltpu.VMEM((asked, width), f32),
            pltpu.VMEM((asked, width), f32),
            pltpu.VMEM((tall, padded), f32),
            pltpu.VMEM((3, low + 8, OUT_Z * chan), f32),
        ],
        operands=10,
        limit=min(60, 18 + 24 * every * asked // (1 << 20)) << 20,
    )(
        gathered, gain, q_weight, kv_weight, out_weight, upx, jnp.asarray(pick, bf16), inner, outer, weights
    )


def on_device(volume, conv_in, conv_out, norm_gain, q_weight, kv_weight, out_weight, up_weight):
    shape = volume.shape
    bx, by, bz, chan = shape
    counts = tuple(lax.axis_size(axis) for axis in AXES)
    first_w, second_w, upx = band_weights(conv_in, conv_out, up_weight, chan)
    rows, *zfaces = pack_rows(volume, counts)
    zgot = exchange(zfaces, "gz")
    rows, first_w, second_w, upx = lax.optimization_barrier((rows, first_w, second_w, upx))
    ygot = exchange(y_faces(rows, zgot, shape, counts), "gy")
    xgot = exchange(x_faces(rows, zgot, ygot, shape, counts), "gx")
    inner, partial = encode_inner(rows, zgot, ygot, first_w, shape, counts)
    outer, copies = encode_outer(rows, zgot, ygot, xgot, first_w, partial, shape, counts)
    gathered = lax.all_to_all(copies, AXES, 0, 0, tiled=True)
    return attend_and_join(
        gathered, norm_gain[None], q_weight, kv_weight, out_weight, upx, inner, outer, second_w, shape, counts
    )


def solution(mesh):
    placed = (P("gx", "gy", "gz", None), P(), P(), P(), P(), P(), P(), P())
    return jax.shard_map(
        on_device, mesh=mesh, in_specs=placed, out_specs=P("gx", "gy", "gz", None), check_vma=False
    )
```

```python
import numpy as np

import jax
import jax.numpy as jnp
from jax import lax
from jax.experimental import pallas as pl
from jax.experimental.pallas import tpu as pltpu
from jax.sharding import PartitionSpec as P

HEADS = 8
AXES = ("gx", "gy", "gz")
OUT_Z = 6
IN_Z = 8
GROUPS = 2

f32 = jnp.float32
bf16 = jnp.bfloat16


def paired(count):
    return count > 2 and count % 2 == 0


def sends(low, high, index, count):
    if count <= 2:
        return [jnp.where(index == 0, high, low)]
    if not paired(count):
        return [high, low]
    even = index % 2 == 0
    return [jnp.where(even, high, low), jnp.where(even, low, high)]


def exchange(faces, axis):
    count = lax.axis_size(axis)
    if count == 1:
        return list(faces)
    if count == 2:
        return [lax.ppermute(faces[0], axis, [(0, 1), (1, 0)])]
    if not paired(count):
        up = [(i, (i + 1) % count) for i in range(count)]
        return [
            lax.ppermute(faces[0], axis, up),
            lax.ppermute(faces[1], axis, [(j, i) for i, j in up]),
        ]
    return [
        lax.ppermute(faces[0], axis, [(i, i ^ 1) for i in range(count)]),
        lax.ppermute(
            faces[1],
            axis,
            [(i, (i + 1) % count if i % 2 else (i - 1) % count) for i in range(count)],
        ),
    ]


def received(got, index, count):
    if len(got) == 1:
        return got[0], got[0]
    if not paired(count):
        return got[0], got[1]
    even = index % 2 == 0
    return jnp.where(even, got[1], got[0]), jnp.where(even, got[0], got[1])


def call(body, outs, scratch=(), operands=0, limit=16 << 20, **more):
    return pl.pallas_call(
        body,
        out_shape=outs,
        in_specs=[pl.BlockSpec(memory_space=pltpu.VMEM)] * operands,
        scratch_shapes=list(scratch),
        compiler_params=pltpu.CompilerParams(vmem_limit_bytes=limit),
        name=body.__name__,
        **more,
    )


def band_weights(kernel_in, kernel_out, up_weight, chan):
    width = up_weight.shape[0]

    def spread_weights(kin, kout, up, first, second, upx):
        for source, target in ((kin, first), (kout, second)):
            target[...] = jnp.zeros(target.shape, target.dtype)
            for tap in range(9):
                block = source[tap]
                for z in range(OUT_Z):
                    target[tap, z * chan : (z + 3) * chan, z * chan : (z + 1) * chan] = block
        for a in range(2):
            pieces = []
            for b in range(2):
                for c in range(2):
                    start = (a * 4 + b * 2 + c) * chan
                    pieces += [up[:, start : start + chan]] * 4
            upx[a] = jnp.concatenate(pieces, axis=1)

    banded = jax.ShapeDtypeStruct((9, IN_Z * chan, OUT_Z * chan), bf16)
    return call(
        spread_weights,
        (banded, banded, jax.ShapeDtypeStruct((2, width, 16 * chan), bf16)),
        operands=3,
    )(
        kernel_in.reshape(9, 3 * chan, chan),
        kernel_out.reshape(9, 3 * chan, chan),
        up_weight,
    )


def y_faces(volume, counts):
    bx, by, bz, chan = volume.shape
    many = 1 if counts[1] <= 2 else 2

    def y_face(vol, *refs):
        outs, (here, arrived) = refs[:many], refs[many:]
        copies = [
            pltpu.make_async_copy(vol.at[:, pl.ds(y, 2)], here.at[side], arrived.at[side])
            for side, y in enumerate((0, by - 2))
        ]
        for copy in copies:
            copy.start()
        for copy in copies:
            copy.wait()
        low, high = (here[side].astype(f32).reshape(bx * 2, bz * chan) for side in range(2))
        for ref, face in zip(outs, sends(low, high, lax.axis_index("gy"), counts[1])):
            ref[...] = face.astype(bf16)

    return pl.pallas_call(
        y_face,
        out_shape=(jax.ShapeDtypeStruct((bx * 2, bz * chan), bf16),) * many,
        in_specs=[pl.BlockSpec(memory_space=pltpu.HBM)],
        scratch_shapes=[pltpu.VMEM((2, bx, 2, bz, chan), bf16), pltpu.SemaphoreType.DMA((2,))],
        compiler_params=pltpu.CompilerParams(vmem_limit_bytes=16 << 20),
        name="y_face",
    )(pltpu.with_memory_space_constraint(volume, pltpu.HBM))


def pack_rows(volume):
    bx, by, bz, chan = volume.shape

    def pack(vol, rows):
        rows[...] = vol[...].reshape(bx * by, bz * chan)

    return call(pack, jax.ShapeDtypeStruct((bx * by, bz * chan), bf16), operands=1)(volume)


def z_faces(rows, ygot, shape, counts):
    bx, by, bz, chan = shape
    many = 1 if counts[2] <= 2 else 2
    yparts = len(ygot)
    half = bx * by // 2

    def z_face(own, *refs):
        yvals, outs = [r[...].astype(f32) for r in refs[:yparts]], refs[yparts:]

        def face(start):
            sides = []
            for side in range(2):
                at = slice(start, start + 2 * chan)
                body = own[side * half : (side + 1) * half, at].astype(f32)
                edges = [v[side * bx : (side + 1) * bx, at] for v in yvals]
                sides.append(jnp.concatenate([body] + edges, axis=0))
            return jnp.concatenate(sides, axis=1)

        faces = sends(face(0), face((bz - 2) * chan), lax.axis_index("gz"), counts[2])
        for ref, value in zip(outs, faces):
            ref[...] = value.astype(bf16)

    out = jax.ShapeDtypeStruct((half + bx * yparts, 4 * chan), bf16)
    return call(z_face, (out,) * many, operands=1 + yparts)(rows, *ygot)


def full_rows(own, zrefs, plane, shape, count):
    bx, by, bz, chan = shape
    side, at = divmod(plane, bx // 2)
    parts = [
        r[at * by : (at + 1) * by, side * 2 * chan : (side + 1) * 2 * chan].astype(f32) for r in zrefs
    ]
    zm, zp = received(parts, lax.axis_index("gz"), count)
    return jnp.concatenate([zm, own[plane * by : (plane + 1) * by, :].astype(f32), zp], axis=1)


def full_edges(yrefs, zrefs, plane, shape, count):
    bx, by, bz, chan = shape
    side, at = divmod(plane, bx // 2)
    out = []
    for i, ref in enumerate(yrefs):
        first = i * bx + 2 * at
        parts = [
            r[bx * by // 2 :, :].astype(f32)[
                first : first + 2, side * 2 * chan : (side + 1) * 2 * chan
            ]
            for r in zrefs
        ]
        zm, zp = received(parts, lax.axis_index("gz"), count)
        own = ref[...].astype(f32)[2 * plane : 2 * plane + 2]
        out.append(jnp.concatenate([zm, own, zp], axis=1))
    return out


def x_faces(rows, zgot, ygot, shape, counts):
    bx, by, bz, chan = shape
    lanes = (bz + 4) * chan
    zparts, yparts = len(zgot), len(ygot)
    many = 1 if counts[0] <= 2 else 2
    tall = 2 * by + 4 * yparts

    def x_face(own, *refs):
        zrefs, yrefs, outs = refs[:zparts], refs[zparts : zparts + yparts], refs[zparts + yparts :]

        def face(first):
            body = [full_rows(own, zrefs, first + q, shape, counts[2]) for q in range(2)]
            edges = [full_edges(yrefs, zrefs, first + q, shape, counts[2]) for q in range(2)]
            return jnp.concatenate(
                body + [edges[q][i] for i in range(yparts) for q in range(2)], axis=0
            )

        for ref, value in zip(outs, sends(face(0), face(bx - 2), lax.axis_index("gx"), counts[0])):
            ref[...] = value.astype(bf16)

    face = jax.ShapeDtypeStruct((tall, lanes), bf16)
    return call(x_face, (face,) * many, operands=1 + zparts + yparts)(rows, *zgot, *ygot)


def banded_conv(source, weights, sums, blocks, starts, rows, stride, chan, first_sum=0):
    outs = []
    tall = rows * len(starts)
    for block in range(blocks):
        lane = block * OUT_Z * chan
        for dy in range(3):
            total = None
            for dx in range(3):
                pieces = [
                    source[at + dx * stride : at + dx * stride + rows, lane : lane + IN_Z * chan]
                    for at in starts
                ]
                piece = pieces[0] if len(pieces) == 1 else jnp.concatenate(pieces, axis=0)
                part = jnp.dot(
                    piece.astype(bf16), weights[dx * 3 + dy], preferred_element_type=f32
                )
                total = part if total is None else total + part
            sums[first_sum + block * 3 + dy, :tall, :] = total
        at = first_sum + block * 3
        outs.append(
            sums[at, 0:tall, :] + sums[at + 1, 1 : tall + 1, :] + sums[at + 2, 2 : tall + 2, :]
        )
    return outs


def put_plane(grid, row, own, zrefs, yrefs, plane, shape, counts):
    bx, by, bz, chan = shape
    nx, ny, nz = counts
    iy, iz = lax.axis_index("gy"), lax.axis_index("gz")
    lane = lax.broadcasted_iota(jnp.int32, (1, (bz + 4) * chan), 1)
    z_ok = ((lane >= 2 * chan) | (iz > 0)) & ((lane < (bz + 2) * chan) | (iz < nz - 1))
    full = full_rows(own, zrefs, plane, shape, nz)
    grid[row + 2 : row + 2 + by, :] = jnp.where(z_ok, full, 0.0)
    ym, yp = received(full_edges(yrefs, zrefs, plane, shape, nz), iy, ny)
    grid[row : row + 2, :] = jnp.where(z_ok & (iy > 0), ym, 0.0)
    grid[row + by + 2 : row + by + 4, :] = jnp.where(z_ok & (iy < ny - 1), yp, 0.0)


def relu_rows(outs):
    return jnp.maximum(jnp.concatenate(outs, axis=1), 0.0).astype(bf16)


def encode_inner(rows, zgot, ygot, weights, shape, counts):
    bx, by, bz, chan = shape
    lanes = (bz + 4) * chan
    stride = by + 8
    tall = (bx - 2) * stride
    groups = bx // 4
    zparts, yparts = len(zgot), len(ygot)

    def encode_middle(own, *refs):
        zrefs, refs = refs[:zparts], refs[zparts:]
        yrefs, (w, enc, partial, grid, sums) = refs[:yparts], refs[yparts:]
        for p in range(bx):
            put_plane(grid, p * stride, own, zrefs, yrefs, p, shape, counts)
        outs = banded_conv(grid, w, sums, (bz + 2) // OUT_Z, [0], tall, stride, chan)
        encoded = relu_rows(outs)
        enc[...] = encoded
        cells = encoded.astype(f32)
        for group in range(groups):
            total = None
            for x in range(max(1, 4 * group), min(bx - 1, 4 * group + 4)):
                plane = cells[(x - 1) * stride : x * stride]
                total = plane if total is None else total + plane
            partial[group * stride : (group + 1) * stride, :] = total

    return call(
        encode_middle,
        (
            jax.ShapeDtypeStruct((tall, (bz + 2) * chan), bf16),
            jax.ShapeDtypeStruct((groups * stride, (bz + 2) * chan), f32),
        ),
        scratch=[
            pltpu.VMEM((bx * stride, lanes), f32),
            pltpu.VMEM((3 * ((bz + 2) // OUT_Z), tall + 8, OUT_Z * chan), f32),
        ],
        operands=2 + zparts + yparts,
    )(rows, *zgot, *ygot, weights)


def encode_outer(rows, zgot, ygot, xgot, weights, partial, shape, counts):
    bx, by, bz, chan = shape
    nx, ny, nz = counts
    lanes = (bz + 4) * chan
    stride = by + 8
    tall = 4 * stride
    groups = bx // 4
    ti, tj, tk = bx // 8, by // 8, bz // 8
    tokens = ti * tj * tk
    width = 8 * chan
    zparts, yparts, xparts = len(zgot), len(ygot), len(xgot)
    devices = nx * ny * nz

    def encode_ends(own, *refs):
        zrefs, refs = refs[:zparts], refs[zparts:]
        yrefs, refs = refs[:yparts], refs[yparts:]
        xrefs, refs = refs[:xparts], refs[xparts:]
        w, part_ref, enc, tok_copies, grid, sums, plane_sum = refs
        ix, iy, iz = (lax.axis_index(axis) for axis in AXES)
        lane = lax.broadcasted_iota(jnp.int32, (1, lanes), 1)
        z_ok = ((lane >= 2 * chan) | (iz > 0)) & ((lane < (bz + 2) * chan) | (iz < nz - 1))
        for slot, plane in ((2, 0), (3, 1), (4, bx - 2), (5, bx - 1)):
            put_plane(grid, slot * stride, own, zrefs, yrefs, plane, shape, counts)
        xm, xp = received([r[...].astype(f32) for r in xrefs], ix, nx)
        for face, first, ok in ((xm, 0, ix > 0), (xp, 6, ix < nx - 1)):
            good = z_ok & ok
            for q in range(2):
                base = (first + q) * stride
                grid[base + 2 : base + 2 + by, :] = jnp.where(good, face[q * by : (q + 1) * by], 0.0)
                at = 2 * by + 2 * q
                ym, yp = received([face[at + 4 * i : at + 4 * i + 2] for i in range(yparts)], iy, ny)
                grid[base : base + 2, :] = jnp.where(good & (iy > 0), ym, 0.0)
                grid[base + by + 2 : base + by + 4, :] = jnp.where(good & (iy < ny - 1), yp, 0.0)
        outs = banded_conv(
            grid, w, sums, (bz + 2) // OUT_Z, [0, 4 * stride], 2 * stride, stride, chan
        )
        encoded = relu_rows(outs)
        enc[...] = encoded
        first_plane = encoded[stride : 2 * stride].astype(f32)
        last_plane = encoded[2 * stride : 3 * stride].astype(f32)
        rows_of = {}
        for i in range(ti):
            features = {}
            for a in range(2):
                group = 2 * i + a
                acc = part_ref[group * stride : (group + 1) * stride, :]
                if group == 0:
                    acc = acc + first_plane
                if group == groups - 1:
                    acc = acc + last_plane
                for g in range(2 * tk):
                    at = (1 + 4 * g) * chan
                    plane_sum[g] = acc[:, at : at + 4 * chan]
                for b in range(2):
                    for g in range(2 * tk):
                        part = None
                        for q in range(4):
                            line = plane_sum[g, pl.ds(1 + 4 * b + q, tj, stride=8), :]
                            part = line if part is None else part + line
                        s = part[:, :chan]
                        for q in range(1, 4):
                            s = s + part[:, q * chan : (q + 1) * chan]
                        features[a, b, g] = s * (1.0 / 64.0)
            for k in range(tk):
                rows_of[i, k] = jnp.concatenate(
                    [features[a, b, 2 * k + c] for a in range(2) for b in range(2) for c in range(2)],
                    axis=1,
                )
        own_tokens = jnp.concatenate([rows_of[i, k] for i in range(ti) for k in range(tk)], axis=0)
        for device in range(devices):
            tok_copies[device] = own_tokens

    return call(
        encode_ends,
        (
            jax.ShapeDtypeStruct((tall, (bz + 2) * chan), bf16),
            jax.ShapeDtypeStruct((devices, tokens, width), f32),
        ),
        scratch=[
            pltpu.VMEM((8 * stride, lanes), f32),
            pltpu.VMEM((3 * ((bz + 2) // OUT_Z), tall + 8, OUT_Z * chan), f32),
            pltpu.VMEM((2 * tk, stride, 4 * chan), f32),
        ],
        operands=3 + zparts + yparts + xparts,
        limit=(16 if devices <= 64 else 32) << 20,
    )(rows, *zgot, *ygot, *xgot, weights, partial)


def sub_blocks(extent):
    out = [(0, 1, -1, extent // 8 - 1, 1)]
    for s in range(extent // 4):
        out.append((1 + 4 * s, 4, 0, s // 2, s % 2))
    out.append((extent + 1, 1, 1, 0, 0))
    return out


def attend_and_join(
    gathered, gain, q_weight, kv_weight, out_weight, upx, inner, outer, weights, shape, counts
):
    bx, by, bz, chan = shape
    nx, ny, nz = counts
    stride = by + 8
    tall = (bx + 2) * stride
    planes = bx // GROUPS
    ti, tj, tk = bx // 8, by // 8, bz // 8
    tokens = ti * tj * tk
    width = 8 * chan
    every = gathered.shape[0] * tokens
    runs, place = [], {}
    for dx in (-1, 0, 1):
        for dy in (-1, 0, 1):
            for dz in (-1, 0, 1):
                for i in {-1: [ti - 1], 0: range(ti), 1: [0]}[dx]:
                    for k in {-1: [tk - 1], 0: range(tk), 1: [0]}[dz]:
                        j0, j1 = {-1: (tj - 1, tj), 0: (0, tj), 1: (0, 1)}[dy]
                        runs.append(((dx, dy, dz), (i * tk + k) * tj + j0, j1 - j0))
                        for j in range(j0, j1):
                            place[dx, dy, dz, i, j, k] = len(place)
    asked = -(-len(place) // 16) * 16
    head_size = width // HEADS
    wide = (bz + 2) * chan
    blocks = -(-bz // OUT_Z)
    padded = (blocks * OUT_Z + 2) * chan

    xs = sub_blocks(bx)
    zs = [(-1, tk - 1, (7 * chan, 8 * chan))]
    zs += [(0, k, (0, 8 * chan)) for k in range(tk)]
    zs += [(1, 0, (0, chan))]
    pick = np.zeros((len(xs) * len(zs) * stride, asked), np.float32)
    for xi, (_, _, dx, i, _) in enumerate(xs):
        for zi, (dz, k, _) in enumerate(zs):
            for first, many, dy, j, _ in sub_blocks(by):
                row = (xi * len(zs) + zi) * stride + first
                pick[row : row + many, place[dx, dy, dz, i, j, k]] = 1.0

    def attend(
        g, gain_ref, qw, kvw, ow, upx_ref, sel, enc_in, enc_out, w, out, normed_all, mine, mine_n, grid, sums, done, sent
    ):
        ix, iy, iz = (lax.axis_index(axis) for axis in AXES)
        t = g[...].reshape(every, width)
        center = t - jnp.mean(t, axis=1, keepdims=True)
        spread = jnp.mean(center * center, axis=1, keepdims=True)
        normed = (center * lax.rsqrt(spread + 1e-05) * gain_ref[...]).astype(bf16)
        normed_all[...] = normed.astype(f32)
        kv = jnp.dot(normed, kvw[...], preferred_element_type=f32).astype(bf16)
        keys, values = kv[:, :width], kv[:, width:]
        blocks_of = {}
        row = 0
        for (dx, dy, dz), first, many in runs:
            if (dx, dy, dz) not in blocks_of:
                x = jnp.clip(ix + dx, 0, nx - 1)
                y = jnp.clip(iy + dy, 0, ny - 1)
                z = jnp.clip(iz + dz, 0, nz - 1)
                device = (x * ny + y) * nz + z
                at = pl.multiple_of(device * tokens, 8)
                blocks_of[dx, dy, dz] = g[device], normed_all[pl.ds(at, tokens), :]
            block, normed_block = blocks_of[dx, dy, dz]
            mine[row : row + many, :] = block[first : first + many]
            mine_n[row : row + many, :] = normed_block[first : first + many]
            row += many
        if asked > row:
            mine[row:, :] = jnp.zeros((asked - row, width), f32)
            mine_n[row:, :] = jnp.zeros((asked - row, width), f32)
        q = jnp.dot(mine_n[...].astype(bf16), qw[...], preferred_element_type=f32).astype(bf16)
        lane = lax.broadcasted_iota(jnp.int32, (1, width), 1) // head_size
        stacked = jnp.concatenate(
            [jnp.where(lane == h, q, jnp.zeros_like(q)) for h in range(HEADS)], axis=0
        )
        scores = (
            lax.dot_general(stacked, keys, (((1,), (1,)), ((), ())), preferred_element_type=f32)
            * head_size ** (-0.5)
        )
        e = jnp.exp(scores - jnp.max(scores, axis=1, keepdims=True))
        total = jnp.sum(e, axis=1, keepdims=True)
        ratio = jnp.dot(e.astype(bf16), values, preferred_element_type=f32) / total
        attended = jnp.zeros((asked, width), f32)
        for h in range(HEADS):
            attended = jnp.where(lane == h, ratio[h * asked : (h + 1) * asked], attended)
        mixture = (
            mine[...] + jnp.dot(attended.astype(bf16), ow[...], preferred_element_type=f32)
        ).astype(bf16)
        picked = jnp.dot(sel[...], mixture, preferred_element_type=f32).astype(bf16)

        row = lax.broadcasted_iota(jnp.int32, (stride, 1), 0)
        second_half = ((row + 3) // 4) % 2 == 0
        y_ok = ((row > 0) | (iy > 0)) & ((row < by + 1) | (iy < ny - 1))
        zl = lax.broadcasted_iota(jnp.int32, (1, wide), 1)
        z_ok = ((zl >= chan) | (iz > 0)) & ((zl < (bz + 1) * chan) | (iz < nz - 1))
        ok = y_ok & z_ok
        x_lo, x_hi = ix > 0, ix < nx - 1
        if padded > wide:
            grid[:, wide:] = jnp.zeros((tall, padded - wide), f32)
        step = len(zs) * stride
        for xi, (first, many, _, _, a) in enumerate(xs):
            raised = jnp.dot(
                picked[xi * step : (xi + 1) * step], upx_ref[a], preferred_element_type=f32
            )
            parts = []
            for zi, (_, _, (l0, l1)) in enumerate(zs):
                block = raised[zi * stride : (zi + 1) * stride]
                half = block.shape[1] // 2
                chosen = jnp.where(second_half, block[:, half:], block[:, :half])
                parts.append(chosen[:, l0:l1])
            upward = jnp.concatenate(parts, axis=1)
            for x in range(first, first + many):
                good = ok
                if x == 0:
                    good = ok & x_lo
                if x == bx + 1:
                    good = ok & x_hi
                ref, at = (enc_in, x - 2) if 2 <= x < bx else (enc_out, x if x < 2 else x - bx + 2)
                cells = ref[at * stride : (at + 1) * stride, :].astype(f32)
                grid[x * stride : (x + 1) * stride, :wide] = jnp.where(good, cells + upward, 0.0)
        copies = []
        for part in range(GROUPS):
            first = part * planes
            outs = banded_conv(
                grid, w, sums, blocks, [first * stride], planes * stride, stride, chan, part * 3 * blocks
            )
            final = jnp.concatenate(outs, axis=1)[:, : bz * chan].astype(bf16)
            for x in range(planes):
                done[first + x] = final[x * stride : x * stride + by].reshape(by, bz, chan)
            span = pl.ds(first, planes)
            copies.append(pltpu.make_async_copy(done.at[span], out.at[span], sent.at[part]))
            copies[-1].start()
        for copy in copies:
            copy.wait()

    return call(
        attend,
        jax.ShapeDtypeStruct(shape, bf16),
        scratch=[
            pltpu.VMEM((every, width), f32),
            pltpu.VMEM((asked, width), f32),
            pltpu.VMEM((asked, width), f32),
            pltpu.VMEM((tall, padded), f32),
            pltpu.VMEM((GROUPS * 3 * blocks, planes * stride + 8, OUT_Z * chan), f32),
            pltpu.VMEM(shape, bf16),
            pltpu.SemaphoreType.DMA((GROUPS,)),
        ],
        out_specs=pl.BlockSpec(memory_space=pltpu.HBM),
        operands=10,
        limit=min(60, 18 + 16 * HEADS * every * asked // (1 << 20)) << 20,
    )(
        gathered, gain, q_weight, kv_weight, out_weight, upx, jnp.asarray(pick, bf16), inner, outer, weights
    )


def on_device(volume, conv_in, conv_out, norm_gain, q_weight, kv_weight, out_weight, up_weight):
    shape = volume.shape
    bx, by, bz, chan = shape
    counts = tuple(lax.axis_size(axis) for axis in AXES)
    first_w, second_w, upx = band_weights(conv_in, conv_out, up_weight, chan)
    ygot = exchange(y_faces(volume, counts), "gy")
    rows = pack_rows(volume)
    zgot = exchange(z_faces(rows, ygot, shape, counts), "gz")
    rows, first_w, second_w, upx = lax.optimization_barrier((rows, first_w, second_w, upx))
    xgot = exchange(x_faces(rows, zgot, ygot, shape, counts), "gx")
    inner, partial = encode_inner(rows, zgot, ygot, first_w, shape, counts)
    outer, copies = encode_outer(rows, zgot, ygot, xgot, first_w, partial, shape, counts)
    gathered = lax.all_to_all(copies, AXES, 0, 0, tiled=True)
    return attend_and_join(
        gathered, norm_gain[None], q_weight, kv_weight, out_weight, upx, inner, outer, second_w, shape, counts
    )


def solution(mesh):
    placed = (P("gx", "gy", "gz", None), P(), P(), P(), P(), P(), P(), P())
    return jax.shard_map(
        on_device, mesh=mesh, in_specs=placed, out_specs=P("gx", "gy", "gz", None), check_vma=False
    )
```

```python
import numpy as np

import jax
import jax.numpy as jnp
from jax import lax
from jax.experimental import pallas as pl
from jax.experimental.pallas import tpu as pltpu
from jax.sharding import PartitionSpec as P

HEADS = 8
AXES = ("gx", "gy", "gz")
OUT_Z = 6
IN_Z = 8
STATS = 128
GROUPS = 2

f32 = jnp.float32
bf16 = jnp.bfloat16


def paired(count):
    return count > 2 and count % 2 == 0


def sends(low, high, index, count):
    if count <= 2:
        return [jnp.where(index == 0, high, low)]
    if not paired(count):
        return [high, low]
    even = index % 2 == 0
    return [jnp.where(even, high, low), jnp.where(even, low, high)]


def exchange(faces, axis):
    count = lax.axis_size(axis)
    if count == 1:
        return list(faces)
    if count == 2:
        return [lax.ppermute(faces[0], axis, [(0, 1), (1, 0)])]
    if not paired(count):
        up = [(i, (i + 1) % count) for i in range(count)]
        return [
            lax.ppermute(faces[0], axis, up),
            lax.ppermute(faces[1], axis, [(j, i) for i, j in up]),
        ]
    return [
        lax.ppermute(faces[0], axis, [(i, i ^ 1) for i in range(count)]),
        lax.ppermute(
            faces[1],
            axis,
            [(i, (i + 1) % count if i % 2 else (i - 1) % count) for i in range(count)],
        ),
    ]


def received(got, index, count):
    if len(got) == 1:
        return got[0], got[0]
    if not paired(count):
        return got[0], got[1]
    even = index % 2 == 0
    return jnp.where(even, got[1], got[0]), jnp.where(even, got[0], got[1])


def call(body, outs, scratch=(), operands=0, limit=16 << 20, **more):
    return pl.pallas_call(
        body,
        out_shape=outs,
        in_specs=[pl.BlockSpec(memory_space=pltpu.VMEM)] * operands,
        scratch_shapes=list(scratch),
        compiler_params=pltpu.CompilerParams(vmem_limit_bytes=limit),
        name=body.__name__,
        **more,
    )


def band_weights(kernel_in, kernel_out, up_weight, chan):
    width = up_weight.shape[0]

    def spread_weights(kin, kout, up, first, second, upx):
        for source, target in ((kin, first), (kout, second)):
            target[...] = jnp.zeros(target.shape, target.dtype)
            for tap in range(9):
                block = source[tap]
                for z in range(OUT_Z):
                    target[tap, z * chan : (z + 3) * chan, z * chan : (z + 1) * chan] = block
        for a in range(2):
            pieces = []
            for b in range(2):
                for c in range(2):
                    start = (a * 4 + b * 2 + c) * chan
                    pieces += [up[:, start : start + chan]] * 4
            upx[a] = jnp.concatenate(pieces, axis=1)

    banded = jax.ShapeDtypeStruct((9, IN_Z * chan, OUT_Z * chan), bf16)
    return call(
        spread_weights,
        (banded, banded, jax.ShapeDtypeStruct((2, width, 16 * chan), bf16)),
        operands=3,
    )(
        kernel_in.reshape(9, 3 * chan, chan),
        kernel_out.reshape(9, 3 * chan, chan),
        up_weight,
    )


def y_faces(volume, counts):
    bx, by, bz, chan = volume.shape
    many = 1 if counts[1] <= 2 else 2

    def y_face(vol, *refs):
        outs, (here, arrived) = refs[:many], refs[many:]
        copies = [
            pltpu.make_async_copy(vol.at[:, pl.ds(y, 2)], here.at[side], arrived.at[side])
            for side, y in enumerate((0, by - 2))
        ]
        for copy in copies:
            copy.start()
        for copy in copies:
            copy.wait()
        low, high = (here[side].astype(f32).reshape(bx * 2, bz * chan) for side in range(2))
        for ref, face in zip(outs, sends(low, high, lax.axis_index("gy"), counts[1])):
            ref[...] = face.astype(bf16)

    return pl.pallas_call(
        y_face,
        out_shape=(jax.ShapeDtypeStruct((bx * 2, bz * chan), bf16),) * many,
        in_specs=[pl.BlockSpec(memory_space=pltpu.HBM)],
        scratch_shapes=[pltpu.VMEM((2, bx, 2, bz, chan), bf16), pltpu.SemaphoreType.DMA((2,))],
        compiler_params=pltpu.CompilerParams(vmem_limit_bytes=16 << 20),
        name="y_face",
    )(pltpu.with_memory_space_constraint(volume, pltpu.HBM))


def pack_rows(volume):
    bx, by, bz, chan = volume.shape

    def pack(vol, rows):
        rows[...] = vol[...].reshape(bx * by, bz * chan)

    return call(pack, jax.ShapeDtypeStruct((bx * by, bz * chan), bf16), operands=1)(volume)


def z_faces(rows, ygot, shape, counts):
    bx, by, bz, chan = shape
    many = 1 if counts[2] <= 2 else 2
    yparts = len(ygot)
    half = bx * by // 2

    def z_face(own, *refs):
        yvals, outs = [r[...].astype(f32) for r in refs[:yparts]], refs[yparts:]

        def face(start):
            sides = []
            for side in range(2):
                at = slice(start, start + 2 * chan)
                body = own[side * half : (side + 1) * half, at].astype(f32)
                edges = [v[side * bx : (side + 1) * bx, at] for v in yvals]
                sides.append(jnp.concatenate([body] + edges, axis=0))
            return jnp.concatenate(sides, axis=1)

        faces = sends(face(0), face((bz - 2) * chan), lax.axis_index("gz"), counts[2])
        for ref, value in zip(outs, faces):
            ref[...] = value.astype(bf16)

    out = jax.ShapeDtypeStruct((half + bx * yparts, 4 * chan), bf16)
    return call(z_face, (out,) * many, operands=1 + yparts)(rows, *ygot)


def full_rows(own, zrefs, plane, shape, count):
    bx, by, bz, chan = shape
    side, at = divmod(plane, bx // 2)
    parts = [
        r[at * by : (at + 1) * by, side * 2 * chan : (side + 1) * 2 * chan].astype(f32) for r in zrefs
    ]
    zm, zp = received(parts, lax.axis_index("gz"), count)
    return jnp.concatenate([zm, own[plane * by : (plane + 1) * by, :].astype(f32), zp], axis=1)


def full_edges(yrefs, zrefs, plane, shape, count):
    bx, by, bz, chan = shape
    side, at = divmod(plane, bx // 2)
    out = []
    for i, ref in enumerate(yrefs):
        first = i * bx + 2 * at
        parts = [
            r[bx * by // 2 :, :].astype(f32)[
                first : first + 2, side * 2 * chan : (side + 1) * 2 * chan
            ]
            for r in zrefs
        ]
        zm, zp = received(parts, lax.axis_index("gz"), count)
        own = ref[...].astype(f32)[2 * plane : 2 * plane + 2]
        out.append(jnp.concatenate([zm, own, zp], axis=1))
    return out


def x_faces(rows, zgot, ygot, shape, counts):
    bx, by, bz, chan = shape
    lanes = (bz + 4) * chan
    zparts, yparts = len(zgot), len(ygot)
    many = 1 if counts[0] <= 2 else 2
    tall = 2 * by + 4 * yparts

    def x_face(own, *refs):
        zrefs, yrefs, outs = refs[:zparts], refs[zparts : zparts + yparts], refs[zparts + yparts :]

        def face(first):
            body = [full_rows(own, zrefs, first + q, shape, counts[2]) for q in range(2)]
            edges = [full_edges(yrefs, zrefs, first + q, shape, counts[2]) for q in range(2)]
            return jnp.concatenate(
                body + [edges[q][i] for i in range(yparts) for q in range(2)], axis=0
            )

        for ref, value in zip(outs, sends(face(0), face(bx - 2), lax.axis_index("gx"), counts[0])):
            ref[...] = value.astype(bf16)

    face = jax.ShapeDtypeStruct((tall, lanes), bf16)
    return call(x_face, (face,) * many, operands=1 + zparts + yparts)(rows, *zgot, *ygot)


def banded_conv(source, weights, sums, blocks, starts, rows, stride, chan, first_sum=0):
    outs = []
    tall = rows * len(starts)
    for block in range(blocks):
        lane = block * OUT_Z * chan
        pieces = []
        for dx in range(3):
            runs = [
                source[at + dx * stride : at + dx * stride + rows, lane : lane + IN_Z * chan]
                for at in starts
            ]
            piece = runs[0] if len(runs) == 1 else jnp.concatenate(runs, axis=0)
            pieces.append(piece.astype(bf16))
        for dy in range(3):
            total = None
            for dx in range(3):
                part = jnp.dot(pieces[dx], weights[dx * 3 + dy], preferred_element_type=f32)
                total = part if total is None else total + part
            sums[first_sum + block * 3 + dy, :tall, :] = total
        at = first_sum + block * 3
        outs.append(
            sums[at, 0:tall, :] + sums[at + 1, 1 : tall + 1, :] + sums[at + 2, 2 : tall + 2, :]
        )
    return outs


def put_plane(grid, row, own, zrefs, yrefs, plane, shape, counts):
    bx, by, bz, chan = shape
    nx, ny, nz = counts
    iy, iz = lax.axis_index("gy"), lax.axis_index("gz")
    lane = lax.broadcasted_iota(jnp.int32, (1, (bz + 4) * chan), 1)
    z_ok = ((lane >= 2 * chan) | (iz > 0)) & ((lane < (bz + 2) * chan) | (iz < nz - 1))
    full = full_rows(own, zrefs, plane, shape, nz)
    grid[row + 2 : row + 2 + by, :] = jnp.where(z_ok, full, 0.0)
    ym, yp = received(full_edges(yrefs, zrefs, plane, shape, nz), iy, ny)
    grid[row : row + 2, :] = jnp.where(z_ok & (iy > 0), ym, 0.0)
    grid[row + by + 2 : row + by + 4, :] = jnp.where(z_ok & (iy < ny - 1), yp, 0.0)


def relu_rows(outs):
    return jnp.maximum(jnp.concatenate(outs, axis=1), 0.0).astype(bf16)


def encode_inner(rows, zgot, ygot, weights, shape, counts):
    bx, by, bz, chan = shape
    lanes = (bz + 4) * chan
    stride = by + 8
    tall = (bx - 2) * stride
    groups = bx // 4
    zparts, yparts = len(zgot), len(ygot)

    def encode_middle(own, *refs):
        zrefs, refs = refs[:zparts], refs[zparts:]
        yrefs, (w, enc, partial, grid, sums) = refs[:yparts], refs[yparts:]
        for p in range(bx):
            put_plane(grid, p * stride, own, zrefs, yrefs, p, shape, counts)
        outs = banded_conv(grid, w, sums, (bz + 2) // OUT_Z, [0], tall, stride, chan)
        encoded = relu_rows(outs)
        enc[...] = encoded
        cells = encoded.astype(f32)
        for group in range(groups):
            total = None
            for x in range(max(1, 4 * group), min(bx - 1, 4 * group + 4)):
                plane = cells[(x - 1) * stride : x * stride]
                total = plane if total is None else total + plane
            partial[group * stride : (group + 1) * stride, :] = total

    return call(
        encode_middle,
        (
            jax.ShapeDtypeStruct((tall, (bz + 2) * chan), bf16),
            jax.ShapeDtypeStruct((groups * stride, (bz + 2) * chan), f32),
        ),
        scratch=[
            pltpu.VMEM((bx * stride, lanes), f32),
            pltpu.VMEM((3 * ((bz + 2) // OUT_Z), tall + 8, OUT_Z * chan), f32),
        ],
        operands=2 + zparts + yparts,
    )(rows, *zgot, *ygot, weights)


def thirds(value):
    first = value.astype(bf16)
    second = (value - first.astype(f32)).astype(bf16)
    third = (value - first.astype(f32) - second.astype(f32)).astype(bf16)
    return [first.astype(f32), second.astype(f32), third.astype(f32)]


def encode_outer(rows, zgot, ygot, xgot, weights, partial, gain, shape, counts):
    bx, by, bz, chan = shape
    nx, ny, nz = counts
    lanes = (bz + 4) * chan
    stride = by + 8
    tall = 4 * stride
    groups = bx // 4
    ti, tj, tk = bx // 8, by // 8, bz // 8
    tokens = ti * tj * tk
    width = 8 * chan
    zparts, yparts, xparts = len(zgot), len(ygot), len(xgot)
    devices = nx * ny * nz

    def encode_ends(own, *refs):
        zrefs, refs = refs[:zparts], refs[zparts:]
        yrefs, refs = refs[:yparts], refs[yparts:]
        xrefs, refs = refs[:xparts], refs[xparts:]
        w, part_ref, gain_ref, enc, tok, tok_copies, grid, sums, plane_sum = refs
        ix, iy, iz = (lax.axis_index(axis) for axis in AXES)
        lane = lax.broadcasted_iota(jnp.int32, (1, lanes), 1)
        z_ok = ((lane >= 2 * chan) | (iz > 0)) & ((lane < (bz + 2) * chan) | (iz < nz - 1))
        for slot, plane in ((2, 0), (3, 1), (4, bx - 2), (5, bx - 1)):
            put_plane(grid, slot * stride, own, zrefs, yrefs, plane, shape, counts)
        xm, xp = received([r[...].astype(f32) for r in xrefs], ix, nx)
        for face, first, ok in ((xm, 0, ix > 0), (xp, 6, ix < nx - 1)):
            good = z_ok & ok
            for q in range(2):
                base = (first + q) * stride
                grid[base + 2 : base + 2 + by, :] = jnp.where(good, face[q * by : (q + 1) * by], 0.0)
                at = 2 * by + 2 * q
                ym, yp = received([face[at + 4 * i : at + 4 * i + 2] for i in range(yparts)], iy, ny)
                grid[base : base + 2, :] = jnp.where(good & (iy > 0), ym, 0.0)
                grid[base + by + 2 : base + by + 4, :] = jnp.where(good & (iy < ny - 1), yp, 0.0)
        outs = banded_conv(
            grid, w, sums, (bz + 2) // OUT_Z, [0, 4 * stride], 2 * stride, stride, chan
        )
        encoded = relu_rows(outs)
        enc[...] = encoded
        first_plane = encoded[stride : 2 * stride].astype(f32)
        last_plane = encoded[2 * stride : 3 * stride].astype(f32)
        rows_of = {}
        for i in range(ti):
            features = {}
            for a in range(2):
                group = 2 * i + a
                acc = part_ref[group * stride : (group + 1) * stride, :]
                if group == 0:
                    acc = acc + first_plane
                if group == groups - 1:
                    acc = acc + last_plane
                for g in range(2 * tk):
                    at = (1 + 4 * g) * chan
                    plane_sum[g] = acc[:, at : at + 4 * chan]
                for b in range(2):
                    for g in range(2 * tk):
                        part = None
                        for q in range(4):
                            line = plane_sum[g, pl.ds(1 + 4 * b + q, tj, stride=8), :]
                            part = line if part is None else part + line
                        s = part[:, :chan]
                        for q in range(1, 4):
                            s = s + part[:, q * chan : (q + 1) * chan]
                        features[a, b, g] = s * (1.0 / 64.0)
            for k in range(tk):
                rows_of[i, k] = jnp.concatenate(
                    [features[a, b, 2 * k + c] for a in range(2) for b in range(2) for c in range(2)],
                    axis=1,
                )
        own_tokens = jnp.concatenate([rows_of[i, k] for i in range(ti) for k in range(tk)], axis=0)
        tok[...] = own_tokens
        mean = jnp.mean(own_tokens, axis=1, keepdims=True)
        center = own_tokens - mean
        spread = jnp.mean(center * center, axis=1, keepdims=True) + 1e-05
        normed = center * lax.rsqrt(spread) * gain_ref[...]
        stat_lane = lax.broadcasted_iota(jnp.int32, (tokens, STATS), 1)
        stats = jnp.zeros((tokens, STATS), f32)
        for at, value in enumerate(thirds(mean) + thirds(jnp.sqrt(spread))):
            stats = jnp.where(stat_lane == at, value, stats)
        sent = jnp.concatenate([normed, stats], axis=1).astype(bf16)
        for device in range(devices):
            tok_copies[device] = sent

    return call(
        encode_ends,
        (
            jax.ShapeDtypeStruct((tall, (bz + 2) * chan), bf16),
            jax.ShapeDtypeStruct((tokens, width), f32),
            jax.ShapeDtypeStruct((devices, tokens, width + STATS), bf16),
        ),
        scratch=[
            pltpu.VMEM((8 * stride, lanes), f32),
            pltpu.VMEM((3 * ((bz + 2) // OUT_Z), tall + 8, OUT_Z * chan), f32),
            pltpu.VMEM((2 * tk, stride, 4 * chan), f32),
        ],
        operands=4 + zparts + yparts + xparts,
        limit=(16 if devices <= 64 else 32) << 20,
    )(rows, *zgot, *ygot, *xgot, weights, partial, gain)


def sub_blocks(extent):
    out = [(0, 1, -1, extent // 8 - 1, 1)]
    for s in range(extent // 4):
        out.append((1 + 4 * s, 4, 0, s // 2, s % 2))
    out.append((extent + 1, 1, 1, 0, 0))
    return out


def attend_and_join(
    gathered, own_tokens, gain, q_weight, kv_weight, out_weight, upx, inner, outer, weights, shape, counts
):
    bx, by, bz, chan = shape
    nx, ny, nz = counts
    stride = by + 8
    tall = (bx + 2) * stride
    planes = bx // GROUPS
    ti, tj, tk = bx // 8, by // 8, bz // 8
    tokens = ti * tj * tk
    width = 8 * chan
    every = gathered.shape[0] * tokens
    runs, place = [], {}
    for dx in (-1, 0, 1):
        for dy in (-1, 0, 1):
            for dz in (-1, 0, 1):
                for i in {-1: [ti - 1], 0: range(ti), 1: [0]}[dx]:
                    for k in {-1: [tk - 1], 0: range(tk), 1: [0]}[dz]:
                        j0, j1 = {-1: (tj - 1, tj), 0: (0, tj), 1: (0, 1)}[dy]
                        runs.append(((dx, dy, dz), (i * tk + k) * tj + j0, j1 - j0))
                        for j in range(j0, j1):
                            place[dx, dy, dz, i, j, k] = len(place)
    asked = -(-len(place) // 16) * 16
    head_size = width // HEADS
    wide = (bz + 2) * chan
    blocks = -(-bz // OUT_Z)
    padded = (blocks * OUT_Z + 2) * chan

    xs = sub_blocks(bx)
    zs = [(-1, tk - 1, (7 * chan, 8 * chan))]
    zs += [(0, k, (0, 8 * chan)) for k in range(tk)]
    zs += [(1, 0, (0, chan))]
    pick = np.zeros((len(xs) * len(zs) * stride, asked), np.float32)
    for xi, (_, _, dx, i, _) in enumerate(xs):
        for zi, (dz, k, _) in enumerate(zs):
            for first, many, dy, j, _ in sub_blocks(by):
                row = (xi * len(zs) + zi) * stride + first
                pick[row : row + many, place[dx, dy, dz, i, j, k]] = 1.0

    def attend(
        g, own, gain_ref, qw, kvw, ow, upx_ref, sel, enc_in, enc_out, w, out, mine, mine_n, grid, sums, done, sent
    ):
        ix, iy, iz = (lax.axis_index(axis) for axis in AXES)
        normed = g[:, :, :width].astype(f32).reshape(every, width).astype(bf16)
        kv = jnp.dot(normed, kvw[...], preferred_element_type=f32).astype(bf16)
        keys, values = kv[:, :width], kv[:, width:]
        blocks_of = {}
        row = 0
        for (dx, dy, dz), first, many in runs:
            if (dx, dy, dz) not in blocks_of:
                x = jnp.clip(ix + dx, 0, nx - 1)
                y = jnp.clip(iy + dy, 0, ny - 1)
                z = jnp.clip(iz + dz, 0, nz - 1)
                device = (x * ny + y) * nz + z
                blocks_of[dx, dy, dz] = g[device].astype(f32)
            mine_n[row : row + many, :] = blocks_of[dx, dy, dz][first : first + many]
            row += many
        if asked > row:
            mine_n[row:, :] = jnp.zeros((asked - row, width + STATS), f32)
        stats = mine_n[:, width:]
        stat_lane = lax.broadcasted_iota(jnp.int32, (1, STATS), 1)
        mean = jnp.sum(jnp.where(stat_lane < 3, stats, 0.0), axis=1, keepdims=True)
        deviation = jnp.sum(jnp.where(stat_lane >= 3, stats, 0.0), axis=1, keepdims=True)
        mine[...] = mean + mine_n[:, :width] * (1.0 / gain_ref[...]) * deviation
        home = min(place[at] for at in place if at[:3] == (0, 0, 0))
        mine[home : home + tokens, :] = own[...]
        q = jnp.dot(mine_n[:, :width].astype(bf16), qw[...], preferred_element_type=f32).astype(bf16)
        lane = lax.broadcasted_iota(jnp.int32, (1, width), 1) // head_size
        stacked = jnp.concatenate(
            [jnp.where(lane == h, q, jnp.zeros_like(q)) for h in range(HEADS)], axis=0
        )
        scores = (
            lax.dot_general(stacked, keys, (((1,), (1,)), ((), ())), preferred_element_type=f32)
            * head_size ** (-0.5)
        )
        e = jnp.exp(scores - jnp.max(scores, axis=1, keepdims=True))
        total = jnp.sum(e, axis=1, keepdims=True)
        ratio = jnp.dot(e.astype(bf16), values, preferred_element_type=f32) / total
        attended = jnp.zeros((asked, width), f32)
        for h in range(HEADS):
            attended = jnp.where(lane == h, ratio[h * asked : (h + 1) * asked], attended)
        mixture = (
            mine[...] + jnp.dot(attended.astype(bf16), ow[...], preferred_element_type=f32)
        ).astype(bf16)
        picked = jnp.dot(sel[...], mixture, preferred_element_type=f32).astype(bf16)

        row = lax.broadcasted_iota(jnp.int32, (stride, 1), 0)
        second_half = ((row + 3) // 4) % 2 == 0
        y_ok = ((row > 0) | (iy > 0)) & ((row < by + 1) | (iy < ny - 1))
        zl = lax.broadcasted_iota(jnp.int32, (1, wide), 1)
        z_ok = ((zl >= chan) | (iz > 0)) & ((zl < (bz + 1) * chan) | (iz < nz - 1))
        ok = y_ok & z_ok
        x_lo, x_hi = ix > 0, ix < nx - 1
        if padded > wide:
            grid[:, wide:] = jnp.zeros((tall, padded - wide), f32)
        step = len(zs) * stride
        for xi, (first, many, _, _, a) in enumerate(xs):
            raised = jnp.dot(
                picked[xi * step : (xi + 1) * step], upx_ref[a], preferred_element_type=f32
            )
            parts = []
            for zi, (_, _, (l0, l1)) in enumerate(zs):
                block = raised[zi * stride : (zi + 1) * stride]
                half = block.shape[1] // 2
                chosen = jnp.where(second_half, block[:, half:], block[:, :half])
                parts.append(chosen[:, l0:l1])
            upward = jnp.concatenate(parts, axis=1)
            for x in range(first, first + many):
                good = ok
                if x == 0:
                    good = ok & x_lo
                if x == bx + 1:
                    good = ok & x_hi
                ref, at = (enc_in, x - 2) if 2 <= x < bx else (enc_out, x if x < 2 else x - bx + 2)
                cells = ref[at * stride : (at + 1) * stride, :].astype(f32)
                grid[x * stride : (x + 1) * stride, :wide] = jnp.where(good, cells + upward, 0.0)
        copies = []
        for part in range(GROUPS):
            first = part * planes
            outs = banded_conv(
                grid, w, sums, blocks, [first * stride], planes * stride, stride, chan, part * 3 * blocks
            )
            final = jnp.concatenate(outs, axis=1)[:, : bz * chan].astype(bf16)
            for x in range(planes):
                done[first + x] = final[x * stride : x * stride + by].reshape(by, bz, chan)
            span = pl.ds(first, planes)
            copies.append(pltpu.make_async_copy(done.at[span], out.at[span], sent.at[part]))
            copies[-1].start()
        for copy in copies:
            copy.wait()

    return call(
        attend,
        jax.ShapeDtypeStruct(shape, bf16),
        scratch=[
            pltpu.VMEM((asked, width), f32),
            pltpu.VMEM((asked, width + STATS), f32),
            pltpu.VMEM((tall, padded), f32),
            pltpu.VMEM((GROUPS * 3 * blocks, planes * stride + 8, OUT_Z * chan), f32),
            pltpu.VMEM(shape, bf16),
            pltpu.SemaphoreType.DMA((GROUPS,)),
        ],
        out_specs=pl.BlockSpec(memory_space=pltpu.HBM),
        operands=11,
        limit=min(60, 18 + 16 * HEADS * every * asked // (1 << 20)) << 20,
    )(
        gathered, own_tokens, gain, q_weight, kv_weight, out_weight, upx, jnp.asarray(pick, bf16), inner, outer, weights
    )


def on_device(volume, conv_in, conv_out, norm_gain, q_weight, kv_weight, out_weight, up_weight):
    shape = volume.shape
    bx, by, bz, chan = shape
    counts = tuple(lax.axis_size(axis) for axis in AXES)
    first_w, second_w, upx = band_weights(conv_in, conv_out, up_weight, chan)
    ygot = exchange(y_faces(volume, counts), "gy")
    rows = pack_rows(volume)
    zgot = exchange(z_faces(rows, ygot, shape, counts), "gz")
    rows, first_w, second_w, upx = lax.optimization_barrier((rows, first_w, second_w, upx))
    xgot = exchange(x_faces(rows, zgot, ygot, shape, counts), "gx")
    inner, partial = encode_inner(rows, zgot, ygot, first_w, shape, counts)
    gain = norm_gain[None]
    outer, tokens, copies = encode_outer(
        rows, zgot, ygot, xgot, first_w, partial, gain, shape, counts
    )
    gathered = lax.all_to_all(copies, AXES, 0, 0, tiled=True)
    return attend_and_join(
        gathered, tokens, gain, q_weight, kv_weight, out_weight, upx, inner, outer, second_w, shape, counts
    )


def solution(mesh):
    placed = (P("gx", "gy", "gz", None), P(), P(), P(), P(), P(), P(), P())
    return jax.shard_map(
        on_device, mesh=mesh, in_specs=placed, out_specs=P("gx", "gy", "gz", None), check_vma=False
    )
```

```python
import numpy as np


import jax
import jax.numpy as jnp
from jax import lax
from jax.experimental import pallas as pl
from jax.experimental.pallas import tpu as pltpu
from jax.sharding import PartitionSpec as P

HEADS = 8
AXES = ("gx", "gy", "gz")
OUT_Z = 6
IN_Z = 8
STATS = 128
GROUPS = 2

f32 = jnp.float32
bf16 = jnp.bfloat16


def paired(count):
    return count > 2 and count % 2 == 0


def sends(low, high, index, count):
    if count <= 2:
        return [jnp.where(index == 0, high, low)]
    if not paired(count):
        return [high, low]
    even = index % 2 == 0
    return [jnp.where(even, high, low), jnp.where(even, low, high)]


def exchange(faces, axis):
    count = lax.axis_size(axis)
    if count == 1:
        return list(faces)
    if count == 2:
        return [lax.ppermute(faces[0], axis, [(0, 1), (1, 0)])]
    if not paired(count):
        up = [(i, (i + 1) % count) for i in range(count)]
        return [
            lax.ppermute(faces[0], axis, up),
            lax.ppermute(faces[1], axis, [(j, i) for i, j in up]),
        ]
    near = lax.ppermute(faces[0], axis, [(i, i ^ 1) for i in range(count)])
    far = lax.ppermute(
        faces[1],
        axis,
        [(i, (i + 1) % count if i % 2 else (i - 1) % count) for i in range(count)],
    )
    return [near, far]


def received(got, index, count):
    if len(got) == 1:
        return got[0], got[0]
    if not paired(count):
        return got[0], got[1]
    even = index % 2 == 0
    return jnp.where(even, got[1], got[0]), jnp.where(even, got[0], got[1])


def call(body, outs, scratch=(), operands=0, limit=16 << 20, **more):
    return pl.pallas_call(
        body,
        out_shape=outs,
        in_specs=[pl.BlockSpec(memory_space=pltpu.VMEM)] * operands,
        scratch_shapes=list(scratch),
        compiler_params=pltpu.CompilerParams(vmem_limit_bytes=limit),
        **more,
    )


def band_weights(kernel_in, kernel_out, up_weight, chan):
    width = up_weight.shape[0]

    def spread_weights(kin, kout, up, first, second, upx):
        for source, target in ((kin, first), (kout, second)):
            target[...] = jnp.zeros(target.shape, target.dtype)
            for tap in range(9):
                block = source[tap]
                for z in range(OUT_Z):
                    target[tap, z * chan : (z + 3) * chan, z * chan : (z + 1) * chan] = block
        for a in range(2):
            pieces = []
            for b in range(2):
                for c in range(2):
                    start = (a * 4 + b * 2 + c) * chan
                    pieces += [up[:, start : start + chan]] * 4
            upx[a] = jnp.concatenate(pieces, axis=1)

    banded = jax.ShapeDtypeStruct((9, IN_Z * chan, OUT_Z * chan), bf16)
    return call(
        spread_weights,
        (banded, banded, jax.ShapeDtypeStruct((2, width, 16 * chan), bf16)),
        operands=3,
    )(
        kernel_in.reshape(9, 3 * chan, chan),
        kernel_out.reshape(9, 3 * chan, chan),
        up_weight,
    )


def y_faces(volume, counts):
    bx, by, bz, chan = volume.shape
    many = 1 if counts[1] <= 2 else 2

    def y_face(vol, *refs):
        outs, (here, arrived) = refs[:many], refs[many:]
        copies = [
            pltpu.make_async_copy(vol.at[:, pl.ds(y, 2)], here.at[side], arrived.at[side])
            for side, y in enumerate((0, by - 2))
        ]
        for copy in copies:
            copy.start()
        for copy in copies:
            copy.wait()
        low, high = (here[side].astype(f32).reshape(bx * 2, bz * chan) for side in range(2))
        for ref, face in zip(outs, sends(low, high, lax.axis_index("gy"), counts[1])):
            ref[...] = face.astype(bf16)

    return pl.pallas_call(
        y_face,
        out_shape=(jax.ShapeDtypeStruct((bx * 2, bz * chan), bf16),) * many,
        in_specs=[pl.BlockSpec(memory_space=pltpu.HBM)],
        scratch_shapes=[pltpu.VMEM((2, bx, 2, bz, chan), bf16), pltpu.SemaphoreType.DMA((2,))],
        compiler_params=pltpu.CompilerParams(vmem_limit_bytes=16 << 20),
        name="y_face",
    )(pltpu.with_memory_space_constraint(volume, pltpu.HBM))


def pack_rows(volume):
    bx, by, bz, chan = volume.shape

    def pack(vol, rows):
        rows[...] = vol[...].reshape(bx * by, bz * chan)

    return call(pack, jax.ShapeDtypeStruct((bx * by, bz * chan), bf16), operands=1)(volume)


def z_faces(rows, ygot, shape, counts):
    bx, by, bz, chan = shape
    many = 1 if counts[2] <= 2 else 2
    yparts = len(ygot)
    half = bx * by // 2

    def z_face(own, *refs):
        yvals, outs = [r[...].astype(f32) for r in refs[:yparts]], refs[yparts:]

        def face(start):
            sides = []
            for side in range(2):
                at = slice(start, start + 2 * chan)
                body = own[side * half : (side + 1) * half, at].astype(f32)
                edges = [v[side * bx : (side + 1) * bx, at] for v in yvals]
                sides.append(jnp.concatenate([body] + edges, axis=0))
            return jnp.concatenate(sides, axis=1)

        faces = sends(face(0), face((bz - 2) * chan), lax.axis_index("gz"), counts[2])
        for ref, value in zip(outs, faces):
            ref[...] = value.astype(bf16)

    out = jax.ShapeDtypeStruct((half + bx * yparts, 4 * chan), bf16)
    return call(z_face, (out,) * many, operands=1 + yparts)(rows, *ygot)


def full_rows(own, zrefs, plane, shape, count):
    bx, by, _, chan = shape
    side, at = divmod(plane, bx // 2)
    parts = [
        r[at * by : (at + 1) * by, side * 2 * chan : (side + 1) * 2 * chan].astype(f32) for r in zrefs
    ]
    zm, zp = received(parts, lax.axis_index("gz"), count)
    return jnp.concatenate([zm, own[plane * by : (plane + 1) * by, :].astype(f32), zp], axis=1)


def full_edges(yrefs, zrefs, plane, shape, count):
    bx, by, _, chan = shape
    side, at = divmod(plane, bx // 2)
    out = []
    for i, ref in enumerate(yrefs):
        first = i * bx + 2 * at
        parts = [
            r[bx * by // 2 :, :].astype(f32)[
                first : first + 2, side * 2 * chan : (side + 1) * 2 * chan
            ]
            for r in zrefs
        ]
        zm, zp = received(parts, lax.axis_index("gz"), count)
        own = ref[...].astype(f32)[2 * plane : 2 * plane + 2]
        out.append(jnp.concatenate([zm, own, zp], axis=1))
    return out


def x_faces(rows, zgot, ygot, shape, counts):
    bx, by, bz, chan = shape
    lanes = (bz + 4) * chan
    zparts, yparts = len(zgot), len(ygot)
    many = 1 if counts[0] <= 2 else 2
    tall = 2 * by + 4 * yparts

    def x_face(own, *refs):
        zrefs, yrefs, outs = refs[:zparts], refs[zparts : zparts + yparts], refs[zparts + yparts :]

        def face(first):
            body = [full_rows(own, zrefs, first + q, shape, counts[2]) for q in range(2)]
            edges = [full_edges(yrefs, zrefs, first + q, shape, counts[2]) for q in range(2)]
            return jnp.concatenate(
                body + [edges[q][i] for i in range(yparts) for q in range(2)], axis=0
            )

        for ref, value in zip(outs, sends(face(0), face(bx - 2), lax.axis_index("gx"), counts[0])):
            ref[...] = value.astype(bf16)

    face = jax.ShapeDtypeStruct((tall, lanes), bf16)
    return call(x_face, (face,) * many, operands=1 + zparts + yparts)(rows, *zgot, *ygot)


def banded_conv(pieces_of, weights, sums, blocks, tall, chan):
    outs = []
    for block in range(blocks):
        lane = block * OUT_Z * chan
        pieces = []
        for dx in range(3):
            runs = pieces_of(dx, slice(lane, lane + IN_Z * chan))
            piece = runs[0] if len(runs) == 1 else jnp.concatenate(runs, axis=0)
            pieces.append(piece.astype(bf16))
        for dy in range(3):
            total = None
            for dx in range(3):
                part = jnp.dot(pieces[dx], weights[dx * 3 + dy], preferred_element_type=f32)
                total = part if total is None else total + part
            sums[block * 3 + dy, :tall, :] = total
        at = block * 3
        outs.append(
            sums[at, 0:tall, :] + sums[at + 1, 1 : tall + 1, :] + sums[at + 2, 2 : tall + 2, :]
        )
    return outs


def put_plane(grid, row, own, zrefs, yrefs, plane, shape, counts):
    _, by, bz, chan = shape
    _, ny, nz = counts
    iy, iz = lax.axis_index("gy"), lax.axis_index("gz")
    lane = lax.broadcasted_iota(jnp.int32, (1, (bz + 4) * chan), 1)
    z_ok = ((lane >= 2 * chan) | (iz > 0)) & ((lane < (bz + 2) * chan) | (iz < nz - 1))
    full = full_rows(own, zrefs, plane, shape, nz)
    grid[row + 2 : row + 2 + by, :] = jnp.where(z_ok, full, 0.0)
    ym, yp = received(full_edges(yrefs, zrefs, plane, shape, nz), iy, ny)
    grid[row : row + 2, :] = jnp.where(z_ok & (iy > 0), ym, 0.0)
    grid[row + by + 2 : row + by + 4, :] = jnp.where(z_ok & (iy < ny - 1), yp, 0.0)


def relu_rows(outs):
    return jnp.maximum(jnp.concatenate(outs, axis=1), 0.0).astype(bf16)


def encode_inner(rows, zgot, ygot, weights, shape, counts):
    bx, by, bz, chan = shape
    lanes = (bz + 4) * chan
    stride = by + 8
    tall = (bx - 2) * stride
    groups = bx // 4
    zparts, yparts = len(zgot), len(ygot)

    def encode_middle(own, *refs):
        zrefs, refs = refs[:zparts], refs[zparts:]
        yrefs, (w, enc, partial, grid, sums) = refs[:yparts], refs[yparts:]
        for p in range(bx):
            put_plane(grid, p * stride, own, zrefs, yrefs, p, shape, counts)
        outs = banded_conv(
            lambda dx, span: [grid[dx * stride : dx * stride + tall, span]],
            w, sums, (bz + 2) // OUT_Z, tall, chan,
        )
        encoded = relu_rows(outs)
        enc[...] = encoded
        cells = encoded.astype(f32)
        for group in range(groups):
            total = None
            for x in range(max(1, 4 * group), min(bx - 1, 4 * group + 4)):
                plane = cells[(x - 1) * stride : x * stride]
                total = plane if total is None else total + plane
            partial[group * stride : (group + 1) * stride, :] = total

    return call(
        encode_middle,
        (
            jax.ShapeDtypeStruct((tall, (bz + 2) * chan), bf16),
            jax.ShapeDtypeStruct((groups * stride, (bz + 2) * chan), f32),
            jax.ShapeDtypeStruct((bx * stride, lanes), f32),
        ),
        scratch=[
            pltpu.VMEM((3 * ((bz + 2) // OUT_Z), tall + 8, OUT_Z * chan), f32),
        ],
        operands=2 + zparts + yparts,
    )(rows, *zgot, *ygot, weights)


def thirds(value):
    first = value.astype(bf16)
    second = (value - first.astype(f32)).astype(bf16)
    third = (value - first.astype(f32) - second.astype(f32)).astype(bf16)
    return [first.astype(f32), second.astype(f32), third.astype(f32)]


def encode_outer(xgot, weights, partial, middle, gain, shape, counts):
    bx, by, bz, chan = shape
    nx, ny, nz = counts
    lanes = (bz + 4) * chan
    stride = by + 8
    tall = 4 * stride
    groups = bx // 4
    ti, tj, tk = bx // 8, by // 8, bz // 8
    tokens = ti * tj * tk
    width = 8 * chan
    xparts, yparts = len(xgot), 1 if ny <= 2 else 2
    devices = nx * ny * nz

    def encode_ends(*refs):
        xrefs, refs = refs[:xparts], refs[xparts:]
        w, part_ref, own_grid, gain_ref, enc, tok, tok_copies, grid, sums, plane_sum = refs
        ix, iy, iz = (lax.axis_index(axis) for axis in AXES)
        lane = lax.broadcasted_iota(jnp.int32, (1, lanes), 1)
        z_ok = ((lane >= 2 * chan) | (iz > 0)) & ((lane < (bz + 2) * chan) | (iz < nz - 1))
        xm, xp = received([r[...].astype(f32) for r in xrefs], ix, nx)
        for face, first, ok in ((xm, 0, ix > 0), (xp, 2, ix < nx - 1)):
            good = z_ok & ok
            for q in range(2):
                base = (first + q) * stride
                grid[base + 2 : base + 2 + by, :] = jnp.where(good, face[q * by : (q + 1) * by], 0.0)
                at = 2 * by + 2 * q
                ym, yp = received([face[at + 4 * i : at + 4 * i + 2] for i in range(yparts)], iy, ny)
                grid[base : base + 2, :] = jnp.where(good & (iy > 0), ym, 0.0)
                grid[base + by + 2 : base + by + 4, :] = jnp.where(good & (iy < ny - 1), yp, 0.0)

        def plane_rows(x, span):
            if 2 <= x < bx + 2:
                return own_grid[(x - 2) * stride : (x - 1) * stride, span]
            slot = x if x < 2 else x - bx
            return grid[slot * stride : (slot + 1) * stride, span]

        outs = banded_conv(
            lambda dx, span: [plane_rows(x + dx, span) for x in (0, 1, bx, bx + 1)],
            w, sums, (bz + 2) // OUT_Z, tall, chan,
        )
        encoded = relu_rows(outs)
        enc[...] = encoded
        first_plane = encoded[stride : 2 * stride].astype(f32)
        last_plane = encoded[2 * stride : 3 * stride].astype(f32)
        rows_of = {}
        for i in range(ti):
            features = {}
            for a in range(2):
                group = 2 * i + a
                acc = part_ref[group * stride : (group + 1) * stride, :]
                if group == 0:
                    acc = acc + first_plane
                if group == groups - 1:
                    acc = acc + last_plane
                for g in range(2 * tk):
                    at = (1 + 4 * g) * chan
                    plane_sum[g] = acc[:, at : at + 4 * chan]
                for b in range(2):
                    for g in range(2 * tk):
                        part = None
                        for q in range(4):
                            line = plane_sum[g, pl.ds(1 + 4 * b + q, tj, stride=8), :]
                            part = line if part is None else part + line
                        s = part[:, :chan]
                        for q in range(1, 4):
                            s = s + part[:, q * chan : (q + 1) * chan]
                        features[a, b, g] = s * (1.0 / 64.0)
            for k in range(tk):
                rows_of[i, k] = jnp.concatenate(
                    [features[a, b, 2 * k + c] for a in range(2) for b in range(2) for c in range(2)],
                    axis=1,
                )
        own_tokens = jnp.concatenate([rows_of[i, k] for i in range(ti) for k in range(tk)], axis=0)
        tok[...] = own_tokens
        mean = jnp.mean(own_tokens, axis=1, keepdims=True)
        center = own_tokens - mean
        spread = jnp.mean(center * center, axis=1, keepdims=True) + 1e-05
        normed = center * lax.rsqrt(spread) * gain_ref[...]
        stat_lane = lax.broadcasted_iota(jnp.int32, (tokens, STATS), 1)
        stats = jnp.zeros((tokens, STATS), f32)
        for at, value in enumerate(thirds(mean) + thirds(jnp.sqrt(spread))):
            stats = jnp.where(stat_lane == at, value, stats)
        sent = jnp.concatenate([normed, stats], axis=1).astype(bf16)
        for device in range(devices):
            tok_copies[device] = sent

    return call(
        encode_ends,
        (
            jax.ShapeDtypeStruct((tall, (bz + 2) * chan), bf16),
            jax.ShapeDtypeStruct((tokens, width), f32),
            jax.ShapeDtypeStruct((devices, tokens, width + STATS), bf16),
        ),
        scratch=[
            pltpu.VMEM((4 * stride, lanes), f32),
            pltpu.VMEM((3 * ((bz + 2) // OUT_Z), tall + 8, OUT_Z * chan), f32),
            pltpu.VMEM((2 * tk, stride, 4 * chan), f32),
        ],
        operands=4 + xparts,
        limit=(16 if devices <= 64 else 32) << 20,
    )(*xgot, weights, partial, middle, gain)


def sub_blocks(extent):
    out = [(0, 1, -1, extent // 8 - 1, 1)]
    for s in range(extent // 4):
        out.append((1 + 4 * s, 4, 0, s // 2, s % 2))
    out.append((extent + 1, 1, 1, 0, 0))
    return out


def attend_and_join(
    gathered, own_tokens, gain, q_weight, kv_weight, out_weight, upx, inner, outer, weights, shape, counts
):
    bx, by, bz, chan = shape
    nx, ny, nz = counts
    stride = by + 8
    planes = bx // GROUPS
    ti, tj, tk = bx // 8, by // 8, bz // 8
    tokens = ti * tj * tk
    width = 8 * chan
    every = gathered.shape[0] * tokens
    runs, place = [], {}
    for dx in (-1, 0, 1):
        for dy in (-1, 0, 1):
            for dz in (-1, 0, 1):
                for i in {-1: [ti - 1], 0: range(ti), 1: [0]}[dx]:
                    for k in {-1: [tk - 1], 0: range(tk), 1: [0]}[dz]:
                        j0, j1 = {-1: (tj - 1, tj), 0: (0, tj), 1: (0, 1)}[dy]
                        runs.append(((dx, dy, dz), (i * tk + k) * tj + j0, j1 - j0))
                        for j in range(j0, j1):
                            place[dx, dy, dz, i, j, k] = len(place)
    asked = -(-len(place) // 16) * 16
    head_size = width // HEADS
    wide = (bz + 2) * chan
    blocks = -(-bz // OUT_Z)
    padded = (blocks * OUT_Z + 2) * chan

    xs = sub_blocks(bx)
    zs = [(-1, tk - 1, (7 * chan, 8 * chan))]
    zs += [(0, k, (0, 8 * chan)) for k in range(tk)]
    zs += [(1, 0, (0, chan))]
    pick = np.zeros((len(xs) * len(zs) * stride, asked), np.float32)
    for xi, (_, _, dx, i, _) in enumerate(xs):
        for zi, (dz, k, _) in enumerate(zs):
            for first, many, dy, j, _ in sub_blocks(by):
                row = (xi * len(zs) + zi) * stride + first
                pick[row : row + many, place[dx, dy, dz, i, j, k]] = 1.0

    def attend(
        g, own, gain_ref, qw, kvw, ow, upx_ref, sel, enc_in, enc_out, w, out, mine, mine_n, windows, done, sent
    ):
        ix, iy, iz = (lax.axis_index(axis) for axis in AXES)
        normed = g[:, :, :width].astype(f32).reshape(every, width).astype(bf16)
        kv = jnp.dot(normed, kvw[...], preferred_element_type=f32).astype(bf16)
        keys, values = kv[:, :width], kv[:, width:]
        blocks_of = {}
        row = 0
        for (dx, dy, dz), first, many in runs:
            if (dx, dy, dz) not in blocks_of:
                x = jnp.clip(ix + dx, 0, nx - 1)
                y = jnp.clip(iy + dy, 0, ny - 1)
                z = jnp.clip(iz + dz, 0, nz - 1)
                device = (x * ny + y) * nz + z
                blocks_of[dx, dy, dz] = g[device].astype(f32)
            mine_n[row : row + many, :] = blocks_of[dx, dy, dz][first : first + many]
            row += many
        if asked > row:
            mine_n[row:, :] = jnp.zeros((asked - row, width + STATS), f32)
        stats = mine_n[:, width:]
        stat_lane = lax.broadcasted_iota(jnp.int32, (1, STATS), 1)
        mean = jnp.sum(jnp.where(stat_lane < 3, stats, 0.0), axis=1, keepdims=True)
        deviation = jnp.sum(jnp.where(stat_lane >= 3, stats, 0.0), axis=1, keepdims=True)
        mine[...] = mean + mine_n[:, :width] * (1.0 / gain_ref[...]) * deviation
        home = min(place[at] for at in place if at[:3] == (0, 0, 0))
        mine[home : home + tokens, :] = own[...]
        q = jnp.dot(mine_n[:, :width].astype(bf16), qw[...], preferred_element_type=f32).astype(bf16)
        lane = lax.broadcasted_iota(jnp.int32, (1, width), 1) // head_size
        stacked = jnp.concatenate(
            [jnp.where(lane == h, q, jnp.zeros_like(q)) for h in range(HEADS)], axis=0
        )
        scores = (
            lax.dot_general(stacked, keys, (((1,), (1,)), ((), ())), preferred_element_type=f32)
            * head_size ** (-0.5)
        )
        e = jnp.exp(scores - jnp.max(scores, axis=1, keepdims=True))
        total = jnp.sum(e, axis=1, keepdims=True)
        ratio = jnp.dot(e.astype(bf16), values, preferred_element_type=f32) / total
        attended = jnp.zeros((asked, width), f32)
        for h in range(HEADS):
            attended = jnp.where(lane == h, ratio[h * asked : (h + 1) * asked], attended)
        mixture = (
            mine[...] + jnp.dot(attended.astype(bf16), ow[...], preferred_element_type=f32)
        ).astype(bf16)
        picked = jnp.dot(sel[...], mixture, preferred_element_type=f32).astype(bf16)

        row = lax.broadcasted_iota(jnp.int32, (stride, 1), 0)
        second_half = ((row + 3) // 4) % 2 == 0
        y_ok = ((row > 0) | (iy > 0)) & ((row < by + 1) | (iy < ny - 1))
        zl = lax.broadcasted_iota(jnp.int32, (1, wide), 1)
        z_ok = ((zl >= chan) | (iz > 0)) & ((zl < (bz + 1) * chan) | (iz < nz - 1))
        ok = y_ok & z_ok
        x_lo, x_hi = ix > 0, ix < nx - 1
        step = len(zs) * stride
        for xi, (first, many, _, _, a) in enumerate(xs):
            raised = jnp.dot(
                picked[xi * step : (xi + 1) * step], upx_ref[a], preferred_element_type=f32
            )
            parts = []
            for zi, (_, _, (l0, l1)) in enumerate(zs):
                block = raised[zi * stride : (zi + 1) * stride]
                half = block.shape[1] // 2
                chosen = jnp.where(second_half, block[:, half:], block[:, :half])
                parts.append(chosen[:, l0:l1])
            upward = jnp.concatenate(parts, axis=1)
            for x in range(first, first + many):
                good = ok
                if x == 0:
                    good = ok & x_lo
                if x == bx + 1:
                    good = ok & x_hi
                ref, at = (enc_in, x - 2) if 2 <= x < bx else (enc_out, x if x < 2 else x - bx + 2)
                cells = ref[at * stride : (at + 1) * stride, :].astype(f32)
                joined = jnp.where(good, cells + upward, 0.0)
                if padded > wide:
                    joined = jnp.concatenate(
                        [joined, jnp.zeros((stride, padded - wide), f32)], axis=1
                    )
                for block in range(blocks):
                    lane0 = block * OUT_Z * chan
                    window = joined[:, lane0 : lane0 + IN_Z * chan]
                    for dy in range(3):
                        windows[block * 3 + dy, x * by : (x + 1) * by, :] = window[
                            dy : dy + by
                        ].astype(bf16)
        copies = []
        for part in range(GROUPS):
            first = part * planes
            outs = []
            for block in range(blocks):
                total = None
                for dx in range(3):
                    for dy in range(3):
                        piece = windows[
                            block * 3 + dy, (first + dx) * by : (first + dx + planes) * by, :
                        ]
                        one = jnp.dot(piece, w[dx * 3 + dy], preferred_element_type=f32)
                        total = one if total is None else total + one
                outs.append(total)
            final = jnp.concatenate(outs, axis=1)[:, : bz * chan].astype(bf16)
            done[first : first + planes] = final.reshape(planes, by, bz, chan)
            span = pl.ds(first, planes)
            copies.append(pltpu.make_async_copy(done.at[span], out.at[span], sent.at[part]))
            copies[-1].start()
        for copy in copies:
            copy.wait()

    return call(
        attend,
        jax.ShapeDtypeStruct(shape, bf16),
        scratch=[
            pltpu.VMEM((asked, width), f32),
            pltpu.VMEM((asked, width + STATS), f32),
            pltpu.VMEM((3 * blocks, (bx + 2) * by, IN_Z * chan), bf16),
            pltpu.VMEM(shape, bf16),
            pltpu.SemaphoreType.DMA((GROUPS,)),
        ],
        out_specs=pl.BlockSpec(memory_space=pltpu.HBM),
        operands=11,
        limit=min(60, 18 + 16 * HEADS * every * asked // (1 << 20)) << 20,
    )(
        gathered, own_tokens, gain, q_weight, kv_weight, out_weight, upx, jnp.asarray(pick, bf16), inner, outer, weights
    )


def on_device(volume, conv_in, conv_out, norm_gain, q_weight, kv_weight, out_weight, up_weight):
    shape = volume.shape
    _, _, _, chan = shape
    counts = tuple(lax.axis_size(axis) for axis in AXES)
    first_w, second_w, upx = band_weights(conv_in, conv_out, up_weight, chan)
    ygot = exchange(y_faces(volume, counts), "gy")
    rows = pack_rows(volume)
    zgot = exchange(z_faces(rows, ygot, shape, counts), "gz")
    rows, first_w, second_w, upx = lax.optimization_barrier((rows, first_w, second_w, upx))
    xgot = exchange(x_faces(rows, zgot, ygot, shape, counts), "gx")
    inner, partial, middle = encode_inner(rows, zgot, ygot, first_w, shape, counts)
    gain = norm_gain[None]
    outer, tokens, copies = encode_outer(
        xgot, first_w, partial, middle, gain, shape, counts
    )
    gathered = lax.all_to_all(copies, AXES, 0, 0, tiled=True)
    return attend_and_join(
        gathered, tokens, gain, q_weight, kv_weight, out_weight, upx, inner, outer, second_w, shape, counts
    )


def solution(mesh):
    placed = (P("gx", "gy", "gz", None), P(), P(), P(), P(), P(), P(), P())

    return jax.shard_map(on_device, mesh=mesh, in_specs=placed, out_specs=P("gx", "gy", "gz", None), check_vma=False)
```

```python
import numpy as np


import jax
import jax.numpy as jnp
from jax import lax
from jax.experimental import pallas as pl
from jax.experimental.pallas import tpu as pltpu
from jax.sharding import PartitionSpec as P

HEADS = 8
AXES = ("gx", "gy", "gz")
OUT_Z = 6
IN_Z = 8
STATS = 128
GROUPS = 2

f32 = jnp.float32
bf16 = jnp.bfloat16


def paired(count):
    return count > 2 and count % 2 == 0


def sends(low, high, index, count):
    if count <= 2:
        return [jnp.where(index == 0, high, low)]
    if not paired(count):
        return [high, low]
    even = index % 2 == 0
    return [jnp.where(even, high, low), jnp.where(even, low, high)]


def exchange(faces, axis):
    count = lax.axis_size(axis)
    if count == 1:
        return list(faces)
    if count == 2:
        return [lax.ppermute(faces[0], axis, [(0, 1), (1, 0)])]
    if not paired(count):
        up = [(i, (i + 1) % count) for i in range(count)]
        return [
            lax.ppermute(faces[0], axis, up),
            lax.ppermute(faces[1], axis, [(j, i) for i, j in up]),
        ]
    near = lax.ppermute(faces[0], axis, [(i, i ^ 1) for i in range(count)])
    far = lax.ppermute(
        faces[1],
        axis,
        [(i, (i + 1) % count if i % 2 else (i - 1) % count) for i in range(count)],
    )
    return [near, far]


def received(got, index, count):
    if len(got) == 1:
        return got[0], got[0]
    if not paired(count):
        return got[0], got[1]
    even = index % 2 == 0
    return jnp.where(even, got[1], got[0]), jnp.where(even, got[0], got[1])


def call(body, outs, scratch=(), operands=0, limit=16 << 20, **more):
    return pl.pallas_call(
        body,
        out_shape=outs,
        in_specs=[pl.BlockSpec(memory_space=pltpu.VMEM)] * operands,
        scratch_shapes=list(scratch),
        compiler_params=pltpu.CompilerParams(vmem_limit_bytes=limit),
        **more,
    )


def band_weights(kernel_in, kernel_out, up_weight, chan):
    width = up_weight.shape[0]

    def spread_weights(kin, kout, up, first, second, upx):
        for source, target in ((kin, first), (kout, second)):
            target[...] = jnp.zeros(target.shape, target.dtype)
            for tap in range(9):
                block = source[tap]
                for z in range(OUT_Z):
                    target[tap, z * chan : (z + 3) * chan, z * chan : (z + 1) * chan] = block
        for a in range(2):
            pieces = []
            for b in range(2):
                for c in range(2):
                    start = (a * 4 + b * 2 + c) * chan
                    pieces += [up[:, start : start + chan]] * 4
            upx[a] = jnp.concatenate(pieces, axis=1)

    banded = jax.ShapeDtypeStruct((9, IN_Z * chan, OUT_Z * chan), bf16)
    return call(
        spread_weights,
        (banded, banded, jax.ShapeDtypeStruct((2, width, 16 * chan), bf16)),
        operands=3,
    )(
        kernel_in.reshape(9, 3 * chan, chan),
        kernel_out.reshape(9, 3 * chan, chan),
        up_weight,
    )


def y_faces(volume, counts):
    bx, by, bz, chan = volume.shape
    many = 1 if counts[1] <= 2 else 2

    def y_face(vol, *refs):
        outs, (here, arrived) = refs[:many], refs[many:]
        starts = (0, by - 2)
        if counts[1] == 2:
            starts = ((1 - lax.axis_index("gy")) * (by - 2),)
        copies = [
            pltpu.make_async_copy(vol.at[:, pl.ds(y, 2)], here.at[side], arrived.at[side])
            for side, y in enumerate(starts)
        ]
        for copy in copies:
            copy.start()
        for copy in copies:
            copy.wait()
        faces = [here[side].astype(f32).reshape(bx * 2, bz * chan) for side in range(len(starts))]
        if len(faces) == 2:
            faces = sends(faces[0], faces[1], lax.axis_index("gy"), counts[1])
        for ref, face in zip(outs, faces):
            ref[...] = face.astype(bf16)

    return pl.pallas_call(
        y_face,
        out_shape=(jax.ShapeDtypeStruct((bx * 2, bz * chan), bf16),) * many,
        in_specs=[pl.BlockSpec(memory_space=pltpu.HBM)],
        scratch_shapes=[pltpu.VMEM((2, bx, 2, bz, chan), bf16), pltpu.SemaphoreType.DMA((2,))],
        compiler_params=pltpu.CompilerParams(vmem_limit_bytes=16 << 20),
        name="y_face",
    )(pltpu.with_memory_space_constraint(volume, pltpu.HBM))


def pack_rows(volume):
    bx, by, bz, chan = volume.shape

    def pack(vol, rows):
        rows[...] = vol[...].reshape(bx * by, bz * chan)

    return call(pack, jax.ShapeDtypeStruct((bx * by, bz * chan), bf16), operands=1)(volume)


def z_faces(rows, ygot, shape, counts):
    bx, by, bz, chan = shape
    many = 1 if counts[2] <= 2 else 2
    yparts = len(ygot)
    half = bx * by // 2

    def z_face(own, *refs):
        yvals, outs = [r[...].astype(f32) for r in refs[:yparts]], refs[yparts:]

        def face(start):
            sides = []
            for side in range(2):
                at = slice(start, start + 2 * chan)
                body = own[side * half : (side + 1) * half, at].astype(f32)
                edges = [v[side * bx : (side + 1) * bx, at] for v in yvals]
                sides.append(jnp.concatenate([body] + edges, axis=0))
            return jnp.concatenate(sides, axis=1)

        faces = sends(face(0), face((bz - 2) * chan), lax.axis_index("gz"), counts[2])
        for ref, value in zip(outs, faces):
            ref[...] = value.astype(bf16)

    out = jax.ShapeDtypeStruct((half + bx * yparts, 4 * chan), bf16)
    return call(z_face, (out,) * many, operands=1 + yparts)(rows, *ygot)


def full_rows(own, zrefs, plane, shape, count):
    bx, by, _, chan = shape
    side, at = divmod(plane, bx // 2)
    parts = [
        r[at * by : (at + 1) * by, side * 2 * chan : (side + 1) * 2 * chan].astype(f32) for r in zrefs
    ]
    zm, zp = received(parts, lax.axis_index("gz"), count)
    return jnp.concatenate([zm, own[plane * by : (plane + 1) * by, :].astype(f32), zp], axis=1)


def full_edges(yrefs, zrefs, plane, shape, count):
    bx, by, _, chan = shape
    side, at = divmod(plane, bx // 2)
    out = []
    for i, ref in enumerate(yrefs):
        first = i * bx + 2 * at
        parts = [
            r[bx * by // 2 :, :].astype(f32)[
                first : first + 2, side * 2 * chan : (side + 1) * 2 * chan
            ]
            for r in zrefs
        ]
        zm, zp = received(parts, lax.axis_index("gz"), count)
        own = ref[...].astype(f32)[2 * plane : 2 * plane + 2]
        out.append(jnp.concatenate([zm, own, zp], axis=1))
    return out


def x_faces(rows, zgot, ygot, shape, counts):
    bx, by, bz, chan = shape
    lanes = (bz + 4) * chan
    zparts, yparts = len(zgot), len(ygot)
    many = 1 if counts[0] <= 2 else 2
    tall = 2 * by + 4 * yparts

    def x_face(own, *refs):
        zrefs, yrefs, outs = refs[:zparts], refs[zparts : zparts + yparts], refs[zparts + yparts :]

        def face(first):
            body = [full_rows(own, zrefs, first + q, shape, counts[2]) for q in range(2)]
            edges = [full_edges(yrefs, zrefs, first + q, shape, counts[2]) for q in range(2)]
            return jnp.concatenate(
                body + [edges[q][i] for i in range(yparts) for q in range(2)], axis=0
            )

        for ref, value in zip(outs, sends(face(0), face(bx - 2), lax.axis_index("gx"), counts[0])):
            ref[...] = value.astype(bf16)

    face = jax.ShapeDtypeStruct((tall, lanes), bf16)
    return call(x_face, (face,) * many, operands=1 + zparts + yparts)(rows, *zgot, *ygot)


def banded_conv(pieces_of, weights, sums, blocks, tall, chan):
    outs = []
    for block in range(blocks):
        lane = block * OUT_Z * chan
        pieces = []
        for dx in range(3):
            runs = pieces_of(dx, slice(lane, lane + IN_Z * chan))
            piece = runs[0] if len(runs) == 1 else jnp.concatenate(runs, axis=0)
            pieces.append(piece.astype(bf16))
        for dy in range(3):
            total = None
            for dx in range(3):
                part = jnp.dot(pieces[dx], weights[dx * 3 + dy], preferred_element_type=f32)
                total = part if total is None else total + part
            sums[block * 3 + dy, :tall, :] = total
        at = block * 3
        outs.append(
            sums[at, 0:tall, :] + sums[at + 1, 1 : tall + 1, :] + sums[at + 2, 2 : tall + 2, :]
        )
    return outs


def put_plane(grid, row, own, zrefs, yrefs, plane, shape, counts):
    _, by, bz, chan = shape
    _, ny, nz = counts
    iy, iz = lax.axis_index("gy"), lax.axis_index("gz")
    lane = lax.broadcasted_iota(jnp.int32, (1, (bz + 4) * chan), 1)
    z_ok = ((lane >= 2 * chan) | (iz > 0)) & ((lane < (bz + 2) * chan) | (iz < nz - 1))
    full = full_rows(own, zrefs, plane, shape, nz)
    grid[row + 2 : row + 2 + by, :] = jnp.where(z_ok, full, 0.0)
    ym, yp = received(full_edges(yrefs, zrefs, plane, shape, nz), iy, ny)
    grid[row : row + 2, :] = jnp.where(z_ok & (iy > 0), ym, 0.0)
    grid[row + by + 2 : row + by + 4, :] = jnp.where(z_ok & (iy < ny - 1), yp, 0.0)


def relu_rows(outs):
    return jnp.concatenate([jnp.maximum(out, 0.0).astype(bf16) for out in outs], axis=1)


def encode_inner(rows, zgot, ygot, weights, shape, counts):
    bx, by, bz, chan = shape
    lanes = (bz + 4) * chan
    stride = by + 8
    tall = (bx - 2) * stride
    groups = bx // 4
    zparts, yparts = len(zgot), len(ygot)

    def encode_middle(own, *refs):
        zrefs, refs = refs[:zparts], refs[zparts:]
        yrefs, (w, enc, partial, grid, sums) = refs[:yparts], refs[yparts:]
        for p in range(bx):
            put_plane(grid, p * stride, own, zrefs, yrefs, p, shape, counts)
        outs = banded_conv(
            lambda dx, span: [grid[dx * stride : dx * stride + tall, span]],
            w, sums, (bz + 2) // OUT_Z, tall, chan,
        )
        encoded = relu_rows(outs)
        enc[...] = encoded
        cells = encoded.astype(f32)
        for group in range(groups):
            total = None
            for x in range(max(1, 4 * group), min(bx - 1, 4 * group + 4)):
                plane = cells[(x - 1) * stride : x * stride]
                total = plane if total is None else total + plane
            partial[group * stride : (group + 1) * stride, :] = total

    return call(
        encode_middle,
        (
            jax.ShapeDtypeStruct((tall, (bz + 2) * chan), bf16),
            jax.ShapeDtypeStruct((groups * stride, (bz + 2) * chan), f32),
            jax.ShapeDtypeStruct((bx * stride, lanes), f32),
        ),
        scratch=[
            pltpu.VMEM((3 * ((bz + 2) // OUT_Z), tall + 8, OUT_Z * chan), f32),
        ],
        operands=2 + zparts + yparts,
    )(rows, *zgot, *ygot, weights)


def thirds(value):
    first = value.astype(bf16)
    second = (value - first.astype(f32)).astype(bf16)
    third = (value - first.astype(f32) - second.astype(f32)).astype(bf16)
    return [first.astype(f32), second.astype(f32), third.astype(f32)]


def encode_outer(xgot, weights, partial, middle, gain, shape, counts):
    bx, by, bz, chan = shape
    nx, ny, nz = counts
    lanes = (bz + 4) * chan
    stride = by + 8
    tall = 4 * stride
    groups = bx // 4
    ti, tj, tk = bx // 8, by // 8, bz // 8
    tokens = ti * tj * tk
    width = 8 * chan
    xparts, yparts = len(xgot), 1 if ny <= 2 else 2
    devices = nx * ny * nz

    def encode_ends(*refs):
        xrefs, refs = refs[:xparts], refs[xparts:]
        w, part_ref, own_grid, gain_ref, enc, tok, tok_copies, grid, sums, plane_sum = refs
        ix, iy, iz = (lax.axis_index(axis) for axis in AXES)
        lane = lax.broadcasted_iota(jnp.int32, (1, lanes), 1)
        z_ok = ((lane >= 2 * chan) | (iz > 0)) & ((lane < (bz + 2) * chan) | (iz < nz - 1))
        xm, xp = received([r[...].astype(f32) for r in xrefs], ix, nx)
        for face, first, ok in ((xm, 0, ix > 0), (xp, 2, ix < nx - 1)):
            good = z_ok & ok
            for q in range(2):
                base = (first + q) * stride
                grid[base + 2 : base + 2 + by, :] = jnp.where(good, face[q * by : (q + 1) * by], 0.0)
                at = 2 * by + 2 * q
                ym, yp = received([face[at + 4 * i : at + 4 * i + 2] for i in range(yparts)], iy, ny)
                grid[base : base + 2, :] = jnp.where(good & (iy > 0), ym, 0.0)
                grid[base + by + 2 : base + by + 4, :] = jnp.where(good & (iy < ny - 1), yp, 0.0)

        def plane_rows(x, span):
            if 2 <= x < bx + 2:
                return own_grid[(x - 2) * stride : (x - 1) * stride, span]
            slot = x if x < 2 else x - bx
            return grid[slot * stride : (slot + 1) * stride, span]

        outs = banded_conv(
            lambda dx, span: [plane_rows(x + dx, span) for x in (0, 1, bx, bx + 1)],
            w, sums, (bz + 2) // OUT_Z, tall, chan,
        )
        encoded = relu_rows(outs)
        enc[...] = encoded
        first_plane = encoded[stride : 2 * stride].astype(f32)
        last_plane = encoded[2 * stride : 3 * stride].astype(f32)
        rows_of = {}
        for i in range(ti):
            features = {}
            for a in range(2):
                group = 2 * i + a
                acc = part_ref[group * stride : (group + 1) * stride, :]
                if group == 0:
                    acc = acc + first_plane
                if group == groups - 1:
                    acc = acc + last_plane
                for g in range(2 * tk):
                    at = (1 + 4 * g) * chan
                    plane_sum[g] = acc[:, at : at + 4 * chan]
                for b in range(2):
                    for g in range(2 * tk):
                        part = None
                        for q in range(4):
                            line = plane_sum[g, pl.ds(1 + 4 * b + q, tj, stride=8), :]
                            part = line if part is None else part + line
                        s = part[:, :chan]
                        for q in range(1, 4):
                            s = s + part[:, q * chan : (q + 1) * chan]
                        features[a, b, g] = s * (1.0 / 64.0)
            for k in range(tk):
                rows_of[i, k] = jnp.concatenate(
                    [features[a, b, 2 * k + c] for a in range(2) for b in range(2) for c in range(2)],
                    axis=1,
                )
        own_tokens = jnp.concatenate([rows_of[i, k] for i in range(ti) for k in range(tk)], axis=0)
        tok[...] = own_tokens
        mean = jnp.mean(own_tokens, axis=1, keepdims=True)
        center = own_tokens - mean
        spread = jnp.mean(center * center, axis=1, keepdims=True) + 1e-05
        normed = center * lax.rsqrt(spread) * gain_ref[...]
        stat_lane = lax.broadcasted_iota(jnp.int32, (tokens, STATS), 1)
        stats = jnp.zeros((tokens, STATS), f32)
        for at, value in enumerate(thirds(mean) + thirds(jnp.sqrt(spread))):
            stats = jnp.where(stat_lane == at, value, stats)
        sent = jnp.concatenate([normed, stats], axis=1).astype(bf16)
        for device in range(devices):
            tok_copies[device] = sent

    return call(
        encode_ends,
        (
            jax.ShapeDtypeStruct((tall, (bz + 2) * chan), bf16),
            jax.ShapeDtypeStruct((tokens, width), f32),
            jax.ShapeDtypeStruct((devices, tokens, width + STATS), bf16),
        ),
        scratch=[
            pltpu.VMEM((4 * stride, lanes), f32),
            pltpu.VMEM((3 * ((bz + 2) // OUT_Z), tall + 8, OUT_Z * chan), f32),
            pltpu.VMEM((2 * tk, stride, 4 * chan), f32),
        ],
        operands=4 + xparts,
        limit=(16 if devices <= 64 else 32) << 20,
    )(*xgot, weights, partial, middle, gain)


def sub_blocks(extent):
    out = [(0, 1, -1, extent // 8 - 1, 1)]
    for s in range(extent // 4):
        out.append((1 + 4 * s, 4, 0, s // 2, s % 2))
    out.append((extent + 1, 1, 1, 0, 0))
    return out


def attend_and_join(
    gathered, own_tokens, gain, q_weight, kv_weight, out_weight, upx, inner, outer, weights, shape, counts
):
    bx, by, bz, chan = shape
    nx, ny, nz = counts
    stride = by + 8
    planes = bx // GROUPS
    ti, tj, tk = bx // 8, by // 8, bz // 8
    tokens = ti * tj * tk
    width = 8 * chan
    every = gathered.shape[0] * tokens
    runs, place = [], {}
    for dx in (-1, 0, 1):
        for dy in (-1, 0, 1):
            for dz in (-1, 0, 1):
                for i in {-1: [ti - 1], 0: range(ti), 1: [0]}[dx]:
                    for k in {-1: [tk - 1], 0: range(tk), 1: [0]}[dz]:
                        j0, j1 = {-1: (tj - 1, tj), 0: (0, tj), 1: (0, 1)}[dy]
                        runs.append(((dx, dy, dz), (i * tk + k) * tj + j0, j1 - j0))
                        for j in range(j0, j1):
                            place[dx, dy, dz, i, j, k] = len(place)
    asked = -(-len(place) // 16) * 16
    head_size = width // HEADS
    wide = (bz + 2) * chan
    blocks = -(-bz // OUT_Z)
    padded = (blocks * OUT_Z + 2) * chan

    xs = sub_blocks(bx)
    zs = [(-1, tk - 1, (7 * chan, 8 * chan))]
    zs += [(0, k, (0, 8 * chan)) for k in range(tk)]
    zs += [(1, 0, (0, chan))]
    pick = np.zeros((len(xs) * len(zs) * stride, asked), np.float32)
    for xi, (_, _, dx, i, _) in enumerate(xs):
        for zi, (dz, k, _) in enumerate(zs):
            for first, many, dy, j, _ in sub_blocks(by):
                row = (xi * len(zs) + zi) * stride + first
                pick[row : row + many, place[dx, dy, dz, i, j, k]] = 1.0

    def attend(
        g, g_rows, own, gain_ref, qw, kvw, ow, upx_ref, sel, enc_in, enc_out, w, out, mine, mine_n, windows, done, sent
    ):
        ix, iy, iz = (lax.axis_index(axis) for axis in AXES)
        normed = g_rows[:, :width]
        kv = jnp.dot(normed, kvw[...], preferred_element_type=f32).astype(bf16)
        keys, values = kv[:, :width], kv[:, width:]
        blocks_of = {}
        row = 0
        for (dx, dy, dz), first, many in runs:
            if (dx, dy, dz) not in blocks_of:
                x = jnp.clip(ix + dx, 0, nx - 1)
                y = jnp.clip(iy + dy, 0, ny - 1)
                z = jnp.clip(iz + dz, 0, nz - 1)
                device = (x * ny + y) * nz + z
                blocks_of[dx, dy, dz] = g[device].astype(f32)
            mine_n[row : row + many, :] = blocks_of[dx, dy, dz][first : first + many]
            row += many
        if asked > row:
            mine_n[row:, :] = jnp.zeros((asked - row, width + STATS), f32)
        stats = mine_n[:, width:]
        stat_lane = lax.broadcasted_iota(jnp.int32, (1, STATS), 1)
        mean = jnp.sum(jnp.where(stat_lane < 3, stats, 0.0), axis=1, keepdims=True)
        deviation = jnp.sum(jnp.where(stat_lane >= 3, stats, 0.0), axis=1, keepdims=True)
        mine[...] = mean + mine_n[:, :width] * (1.0 / gain_ref[...]) * deviation
        home = min(place[at] for at in place if at[:3] == (0, 0, 0))
        mine[home : home + tokens, :] = own[...]
        q = jnp.dot(mine_n[:, :width].astype(bf16), qw[...], preferred_element_type=f32).astype(bf16)
        lane = lax.broadcasted_iota(jnp.int32, (1, width), 1) // head_size
        stacked = jnp.concatenate(
            [jnp.where(lane == h, q, jnp.zeros_like(q)) for h in range(HEADS)], axis=0
        )
        scores = (
            lax.dot_general(stacked, keys, (((1,), (1,)), ((), ())), preferred_element_type=f32)
            * head_size ** (-0.5)
        )
        e = jnp.exp(scores - jnp.max(scores, axis=1, keepdims=True))
        total = jnp.sum(e, axis=1, keepdims=True)
        num = jnp.dot(e.astype(bf16), values, preferred_element_type=f32)
        top = jnp.zeros((asked, width), f32)
        bottom = jnp.ones((asked, width), f32)
        for h in range(HEADS):
            at = slice(h * asked, (h + 1) * asked)
            top = jnp.where(lane == h, num[at], top)
            bottom = jnp.where(lane == h, total[at], bottom)
        attended = top / bottom
        mixture = (
            mine[...] + jnp.dot(attended.astype(bf16), ow[...], preferred_element_type=f32)
        ).astype(bf16)
        picked = jnp.dot(sel[...], mixture, preferred_element_type=f32).astype(bf16)

        row = lax.broadcasted_iota(jnp.int32, (stride, 1), 0)
        second_half = ((row + 3) // 4) % 2 == 0
        y_ok = ((row > 0) | (iy > 0)) & ((row < by + 1) | (iy < ny - 1))
        zl = lax.broadcasted_iota(jnp.int32, (1, wide), 1)
        z_ok = ((zl >= chan) | (iz > 0)) & ((zl < (bz + 1) * chan) | (iz < nz - 1))
        ok = y_ok & z_ok
        x_lo, x_hi = ix > 0, ix < nx - 1
        step = len(zs) * stride
        for xi, (first, many, _, _, a) in enumerate(xs):
            raised = jnp.dot(
                picked[xi * step : (xi + 1) * step], upx_ref[a], preferred_element_type=f32
            )
            parts = []
            for zi, (_, _, (l0, l1)) in enumerate(zs):
                block = raised[zi * stride : (zi + 1) * stride]
                half = block.shape[1] // 2
                chosen = jnp.where(second_half, block[:, half:], block[:, :half])
                parts.append(chosen[:, l0:l1])
            upward = jnp.concatenate(parts, axis=1)
            for x in range(first, first + many):
                good = ok
                if x == 0:
                    good = ok & x_lo
                if x == bx + 1:
                    good = ok & x_hi
                ref, at = (enc_in, x - 2) if 2 <= x < bx else (enc_out, x if x < 2 else x - bx + 2)
                cells = ref[at * stride : (at + 1) * stride, :].astype(f32)
                joined = jnp.where(good, cells + upward, 0.0)
                if padded > wide:
                    joined = jnp.concatenate(
                        [joined, jnp.zeros((stride, padded - wide), f32)], axis=1
                    )
                for dy in range(3):
                    line = joined[dy : dy + by].astype(bf16)
                    for block in range(blocks):
                        lane0 = block * OUT_Z * chan
                        windows[block * 3 + dy, x * by : (x + 1) * by, :] = line[
                            :, lane0 : lane0 + IN_Z * chan
                        ]
        copies = []
        for part in range(GROUPS):
            first = part * planes
            outs = []
            for block in range(blocks):
                total = None
                for dx in range(3):
                    for dy in range(3):
                        piece = windows[
                            block * 3 + dy, (first + dx) * by : (first + dx + planes) * by, :
                        ]
                        one = jnp.dot(piece, w[dx * 3 + dy], preferred_element_type=f32)
                        total = one if total is None else total + one
                outs.append(total.astype(bf16))
            final = jnp.concatenate(outs, axis=1)[:, : bz * chan]
            done[first : first + planes] = final.reshape(planes, by, bz, chan)
            span = pl.ds(first, planes)
            copies.append(pltpu.make_async_copy(done.at[span], out.at[span], sent.at[part]))
            copies[-1].start()
        for copy in copies:
            copy.wait()

    return call(
        attend,
        jax.ShapeDtypeStruct(shape, bf16),
        scratch=[
            pltpu.VMEM((asked, width), f32),
            pltpu.VMEM((asked, width + STATS), f32),
            pltpu.VMEM((3 * blocks, (bx + 2) * by, IN_Z * chan), bf16),
            pltpu.VMEM(shape, bf16),
            pltpu.SemaphoreType.DMA((GROUPS,)),
        ],
        out_specs=pl.BlockSpec(memory_space=pltpu.HBM),
        operands=12,
        limit=min(60, 18 + 16 * HEADS * every * asked // (1 << 20)) << 20,
    )(
        gathered, gathered.reshape(every, width + STATS), own_tokens, gain, q_weight, kv_weight, out_weight, upx, jnp.asarray(pick, bf16), inner, outer, weights
    )


def on_device(volume, conv_in, conv_out, norm_gain, q_weight, kv_weight, out_weight, up_weight):
    shape = volume.shape
    _, _, _, chan = shape
    counts = tuple(lax.axis_size(axis) for axis in AXES)
    first_w, second_w, upx = band_weights(conv_in, conv_out, up_weight, chan)
    ygot = exchange(y_faces(volume, counts), "gy")
    rows = pack_rows(volume)
    zgot = exchange(z_faces(rows, ygot, shape, counts), "gz")
    rows, first_w, second_w, upx = lax.optimization_barrier((rows, first_w, second_w, upx))
    xgot = exchange(x_faces(rows, zgot, ygot, shape, counts), "gx")
    inner, partial, middle = encode_inner(rows, zgot, ygot, first_w, shape, counts)
    gain = norm_gain[None]
    outer, tokens, copies = encode_outer(
        xgot, first_w, partial, middle, gain, shape, counts
    )
    gathered = lax.all_to_all(copies, AXES, 0, 0, tiled=True)
    return attend_and_join(
        gathered, tokens, gain, q_weight, kv_weight, out_weight, upx, inner, outer, second_w, shape, counts
    )


def solution(mesh):
    placed = (P("gx", "gy", "gz", None), P(), P(), P(), P(), P(), P(), P())

    return jax.shard_map(on_device, mesh=mesh, in_specs=placed, out_specs=P("gx", "gy", "gz", None), check_vma=False)
```
